128 devices in a mesh: dp: 32 (over z, y, core), tensor: 4 (over x).
Axes of the slice: x: 4, y: 4, z: 4, core: 2. Of those that a mesh axis runs over, the one named last changes fastest.
Arguments:
- sampled_earlier_tokens: int32 [128, 169], P('dp'), may hold values from 0 to 4095
- quantizer_vectors: float32 [4096, 32], replicated, may hold values from -6 to 6
- summed_latent_canvas: float32 [128, 256, 32], P('dp'), may hold values from -6 to 6
- latent_lift_matrix: float32 [32, 1536], replicated, may hold values from -1 to 1
- location_tier_offset: float32 [256, 1536], replicated, may hold values from -3 to 3
- adaptive_norm_factors: float32 [1, 128, 6, 1536], P(None, 'dp'), may hold values from -3 to 3
- logit_sharpness: float32 [1, 16], P(None, 'tensor'), may hold values from 2 to 240, as said below
- probe_match_content_matrix: bfloat16 [1, 1536, 3, 1536], P(None, 'dp', None, 'tensor'), may hold values from -1 to 1, as said below
- mixing_projection_matrix: bfloat16 [1, 1536, 1536], P(None, 'tensor', 'dp'), may hold values from -0.15625 to 0.15625
- widening_projection_matrix: bfloat16 [1, 1536, 6144], P(None, 'dp', 'tensor'), may hold values from -0.15625 to 0.15625
- narrowing_projection_matrix: bfloat16 [1, 6144, 1536], P(None, 'tensor', 'dp'), may hold values from -0.078125 to 0.078125
- cached_lower_grid_lookups: bfloat16 [1, 128, 424, 1536], P(None, 'dp', None, 'tensor'), may hold values from -6 to 6
- cached_lower_grid_payloads: bfloat16 [1, 128, 424, 1536], P(None, 'dp', None, 'tensor'), may hold values from -6 to 6
- final_norm_factors: float32 [128, 2, 1536], P('dp'), may hold values from -3 to 3
- vocabulary_logit_matrix: bfloat16 [1536, 4096], P(None, 'tensor'), may hold values from -0.15625 to 0.15625
Outputs:
- logits: bfloat16 [128, 256, 4096], P('dp', None, 'tensor')
- canvas: float32 [128, 256, 32], P('dp')
The draws below stay inside these ranges and needn't reach their ends.
Inputs may be any that keep to these rules, and one draw needn't show every extreme that they name: `logit_sharpness`: Positive. `probe_match_content_matrix`: entries of spread about 1536 ** -0.5.
All inputs are finite; a program needn't handle non-finite values.
Results may differ from the reference program's by a relative error of at most 0.015.
Values may be sent and summed in bfloat16 or wider, within the bound.
A program may use at most 128 MiB of HBM per device.

```python
import math
import jax
import jax.numpy as jnp
from jax import lax

D = 1536
HEADS = 16
HDIM = 96
FF = 6144
VOCAB = 4096
CVAE = 32
LAYERS = 1
SIDE = 16
PREV = 13
CACHE = 424
TOK = 256
PREVTOK = 169
IMAGES = 128
N_TENSOR = 4


def draw_probe_match_content_matrix(key, part):
    base_draw = jax.random.truncated_normal(jax.random.fold_in(key, 11), -6.0, 6.0, (LAYERS, D, 3, D), jnp.float32) * D ** (-0.5)
    drawn_values = base_draw
    return drawn_values.astype(jnp.bfloat16)


def draw_logit_sharpness(key, part):
    exponent = jax.random.uniform(jax.random.fold_in(key, 23), (LAYERS, HEADS), jnp.float32, math.log(2.0), math.log(60.0))
    drawn_values = jnp.exp(exponent)
    return drawn_values


def plant(array, stream_key, least, top_value):
    extent = array.shape
    place = [jax.random.randint(jax.random.fold_in(stream_key, axis), (), 0, extent[axis]) for axis in range(len(extent))]
    array = array.at[tuple(place)].set(least)
    longest = extent.index(max(extent))
    place[longest] = (place[longest] + 1) % extent[longest]
    return array.at[tuple(place)].set(top_value)


def block_levels(key, dims, pieces, smallest, largest):
    factor_of = 1.0
    for dim, parts in pieces:
        draws = jax.random.uniform(jax.random.fold_in(jax.random.fold_in(key, 6), dim), (parts,), jnp.float32, smallest / len(pieces), largest / len(pieces))
        factor_of = factor_of * jnp.repeat(jnp.exp(draws), dims[dim] // parts).reshape((-1,) + (1,) * (len(dims) - 1 - dim))
    return factor_of


def noise(key, dims, width, bound, cuts=(), kind=jnp.bfloat16):
    array = jax.random.normal(key, dims, jnp.float32) * width
    if len(cuts) > 0:
        array = block_levels(key, dims, cuts, -0.22, 0.18) * array
    return jnp.clip(array, min=-bound, max=bound).astype(kind)


def setup_inputs(seed: int = 0) -> dict:
    streams_of = jax.random.split(jax.random.key(seed), 16)
    return {
        "sampled_earlier_tokens": plant(jax.random.randint(streams_of[0], (IMAGES, PREVTOK), 0, VOCAB), jax.random.fold_in(streams_of[0], 1), 0, VOCAB - 1).astype(jnp.int32),
        "quantizer_vectors": noise(streams_of[1], (VOCAB, CVAE), 1.0, 6.0, (), jnp.float32),
        "summed_latent_canvas": noise(streams_of[2], (IMAGES, TOK, CVAE), 1.0, 6.0, ((0, 32),), jnp.float32),
        "latent_lift_matrix": noise(streams_of[3], (CVAE, D), CVAE ** -0.5, 1.0, (), jnp.float32),
        "location_tier_offset": noise(streams_of[4], (TOK, D), 0.5, 3.0, (), jnp.float32),
        "adaptive_norm_factors": noise(streams_of[5], (LAYERS, IMAGES, 6, D), 0.5, 3.0, ((1, 32),), jnp.float32),
        "logit_sharpness": draw_logit_sharpness(jax.random.fold_in(streams_of[15], 71), 0),
        "probe_match_content_matrix": draw_probe_match_content_matrix(jax.random.fold_in(streams_of[15], 71), 0),
        "mixing_projection_matrix": noise(streams_of[8], (LAYERS, D, D), D ** -0.5, 0.15625, ((1, 4), (2, 32))),
        "widening_projection_matrix": noise(streams_of[9], (LAYERS, D, FF), D ** -0.5, 0.15625, ((1, 32), (2, 4))),
        "narrowing_projection_matrix": noise(streams_of[10], (LAYERS, FF, D), FF ** -0.5, 0.078125, ((1, 4), (2, 32))),
        "cached_lower_grid_lookups": noise(streams_of[11], (LAYERS, IMAGES, CACHE, D), 1.0, 6.0, ((1, 32), (3, 4))),
        "cached_lower_grid_payloads": noise(streams_of[12], (LAYERS, IMAGES, CACHE, D), 1.0, 6.0, ((1, 32), (3, 4))),
        "final_norm_factors": noise(streams_of[13], (IMAGES, 2, D), 0.5, 3.0, ((0, 32),), jnp.float32),
        "vocabulary_logit_matrix": noise(streams_of[14], (D, VOCAB), D ** -0.5, 0.15625, ((1, 4),)),
    }


norm_floor = 0.1
highest = lax.Precision.HIGHEST

def interp_matrix(grid_side, prev_side):
    out_cells = jnp.arange(grid_side, dtype=jnp.int32)
    numerator = jnp.maximum((2 * out_cells + 1) * prev_side - grid_side, 0)
    lower_cell = numerator // (2 * grid_side)
    fraction = (numerator % (2 * grid_side)).astype(jnp.float32) / (2.0 * grid_side)
    upper_cell = jnp.minimum(lower_cell + 1, prev_side - 1)
    in_cells = jnp.arange(prev_side, dtype=jnp.int32)
    lower_hit = (in_cells[None, :] == lower_cell[:, None]).astype(jnp.float32)
    upper_hit = (in_cells[None, :] == upper_cell[:, None]).astype(jnp.float32)
    return lower_hit * (1.0 - fraction)[:, None] + upper_hit * fraction[:, None]

def modulate(stream, scale_vec, shift_vec):
    center = stream - lax.optimization_barrier(jnp.mean(stream, axis=-1, keepdims=True))
    variance = lax.optimization_barrier(jnp.mean(center * center, axis=-1, keepdims=True))
    return center * lax.rsqrt(variance + norm_floor) * (1.0 + scale_vec) + shift_vec

def hidden_neuron_slice(vectors):
    return vectors * lax.rsqrt(lax.optimization_barrier(jnp.sum(vectors * vectors, axis=-1, keepdims=True)) + 1.0)

def group_sum(left_rows, weight, groups):
    part_width = left_rows.shape[1] // groups
    running = jnp.zeros((left_rows.shape[0], weight.shape[1]), jnp.float32)
    for group_id in range(groups):
        partial_value = jnp.dot(left_rows[:, group_id * part_width:(group_id + 1) * part_width], weight[group_id * part_width:(group_id + 1) * part_width], preferred_element_type=jnp.float32)
        rounded = lax.optimization_barrier(partial_value.astype(jnp.bfloat16))
        running = running + rounded.astype(jnp.float32)
    return running

def attend_image(operands):
    probe_token_slab, keys_all, values_all = operands
    scores = jnp.einsum('thd,shd->hts', probe_token_slab.astype(jnp.float32), keys_all.astype(jnp.float32), precision=highest)
    row_max = lax.optimization_barrier(jnp.max(scores, axis=-1, keepdims=True))
    shifted = jnp.exp(scores - row_max)
    weights_bf = (shifted / lax.optimization_barrier(jnp.sum(shifted, axis=-1, keepdims=True))).astype(jnp.bfloat16)
    attended = jnp.einsum('hts,shd->thd', weights_bf.astype(jnp.float32), values_all.astype(jnp.float32), precision=highest)
    return attended.astype(jnp.bfloat16)

def reference(sampled_earlier_tokens, quantizer_vectors, summed_latent_canvas, latent_lift_matrix, location_tier_offset, adaptive_norm_factors, logit_sharpness, probe_match_content_matrix, mixing_projection_matrix, widening_projection_matrix, narrowing_projection_matrix, cached_lower_grid_lookups, cached_lower_grid_payloads, final_norm_factors, vocabulary_logit_matrix):
    vocab_ids = jnp.arange(VOCAB, dtype=jnp.int32)

    def embed_image(token_ids):
        onehot = (token_ids[:, None] == vocab_ids[None, :]).astype(jnp.float32)
        return jnp.dot(onehot, quantizer_vectors, precision=highest, preferred_element_type=jnp.float32)
    embedded = lax.map(embed_image, sampled_earlier_tokens).reshape(IMAGES, PREV, PREV, CVAE)
    up_matrix = interp_matrix(SIDE, PREV)
    lifted = jnp.einsum('ai,nijc->najc', up_matrix, embedded, precision=highest)
    lifted = jnp.einsum('bj,najc->nabc', up_matrix, lifted, precision=highest)
    canvas = summed_latent_canvas + lifted.reshape(IMAGES, TOK, CVAE)
    stream = jnp.einsum('ntc,cd->ntd', canvas, latent_lift_matrix, precision=highest) + location_tier_offset[None]
    for depth_ordinal in range(LAYERS):
        factors = adaptive_norm_factors[depth_ordinal]
        normed = modulate(stream, factors[:, 2][:, None], factors[:, 4][:, None]).astype(jnp.bfloat16)
        projected = jnp.dot(normed.reshape(IMAGES * TOK, D), probe_match_content_matrix[depth_ordinal].reshape(D, 3 * D), preferred_element_type=jnp.float32)
        complete_channel_group_set = projected.reshape(IMAGES, TOK, 3, HEADS, HDIM)
        probe_token_slab = (hidden_neuron_slice(complete_channel_group_set[:, :, 0]) * logit_sharpness[depth_ordinal][None, None, :, None]).astype(jnp.bfloat16)
        key_new = hidden_neuron_slice(complete_channel_group_set[:, :, 1]).astype(jnp.bfloat16)
        value_new = complete_channel_group_set[:, :, 2].astype(jnp.bfloat16)
        key_old = hidden_neuron_slice(cached_lower_grid_lookups[depth_ordinal].astype(jnp.float32).reshape(IMAGES, CACHE, HEADS, HDIM)).astype(jnp.bfloat16)
        value_old = cached_lower_grid_payloads[depth_ordinal].reshape(IMAGES, CACHE, HEADS, HDIM)
        keys_all = jnp.concatenate([key_old, key_new], axis=1)
        values_all = jnp.concatenate([value_old, value_new], axis=1)
        attended = lax.map(attend_image, (probe_token_slab, keys_all, values_all))
        mixed_rows = group_sum(attended.reshape(IMAGES * TOK, D), mixing_projection_matrix[depth_ordinal], N_TENSOR)
        stream = stream + factors[:, 0][:, None] * mixed_rows.reshape(IMAGES, TOK, D)
        normed = modulate(stream, factors[:, 3][:, None], factors[:, 5][:, None]).astype(jnp.bfloat16)
        hidden = jax.nn.gelu(jnp.dot(normed.reshape(IMAGES * TOK, D), widening_projection_matrix[depth_ordinal], preferred_element_type=jnp.float32), approximate=True).astype(jnp.bfloat16)
        mixed_rows = group_sum(hidden, narrowing_projection_matrix[depth_ordinal], N_TENSOR)
        stream = stream + factors[:, 1][:, None] * mixed_rows.reshape(IMAGES, TOK, D)
    normed = modulate(stream, final_norm_factors[:, 0][:, None], final_norm_factors[:, 1][:, None]).astype(jnp.bfloat16)
    logits = jnp.dot(normed.reshape(IMAGES * TOK, D), vocabulary_logit_matrix, preferred_element_type=jnp.float32).astype(jnp.bfloat16)
    return (logits.reshape(IMAGES, TOK, VOCAB), canvas)
```

```python
import numpy as np
import jax
import jax.numpy as jnp
from jax import lax
from jax.experimental import pallas as pl
from jax.experimental.pallas import tpu as pltpu
from jax.sharding import PartitionSpec as P

MESH = pl.DeviceIdType.MESH
BF = jnp.bfloat16
F32 = jnp.float32

D = 1536
HEADS_L = 4
HDIM = 96
LW = HEADS_L * HDIM
VOCAB = 4096
VL = 1024
CVAE = 32
SIDE = 16
PREV = 13
PREVPAD = 176
CACHE = 424
TOK = 256
HALF = 128
IMGS = 4
SH = 48
NX = 4
FLOOR = 0.1

WINDOWS = ((0, 128), (0, 256), (128, 384), (256, 384))

SPLITS = (
    ((0, 640, 384), (640, 1152, 896)),
    ((0, 768, 384), (768, 1536, 1152)),
    ((0, 768, 384), (768, 1536, 1152)),
    ((0, 768, 384), (768, 1536, 1152)),
)


def upsample_matrix():
    a = np.arange(SIDE)
    num = np.maximum((2 * a + 1) * PREV - SIDE, 0)
    low = num // (2 * SIDE)
    frac = (num % (2 * SIDE)) / (2.0 * SIDE)
    up = np.zeros((SIDE, PREV))
    up[a, low] += 1.0 - frac
    up[a, np.minimum(low + 1, PREV - 1)] += frac
    both = np.zeros((TOK, PREVPAD), np.float32)
    both[:, : PREV * PREV] = np.kron(up, up)
    return both


def dot(a, b):
    return jnp.dot(a, b, preferred_element_type=F32)


def dot_nt(a, b):
    return lax.dot_general(a, b, (((1,), (1,)), ((), ())), preferred_element_type=F32)


def pick(index, values):
    out = values[-1]
    for k in range(len(values) - 1):
        out = jnp.where(index == k, values[k], out)
    return out


def body(
    tok_h, quant_h, canvas_h, lift_h, loc_h, fac_h, sharp_s, qkv_h, wo_h, up_h, wd_h,
    kc_h, vc_h, fin_h, voc_h, kron_h,
    logits_h, canvas_o,
    tok, quant, canv, lift, loc, fac, woin, wdin, kc, vc, fin, voc, kron,
    wq, wo, wu, wd,
    emb, cout, st, nb1, nb2, nb3, qn, kn, vn, knc, att, attr, hid, pbuf, precv, lout,
    load_sem, own_sem, out_sem, cout_sem,
    us, ur, wos, wor, ats, atr, g2s, g2r, rss, rsr, g3s, g3r,
):
    me = lax.axis_index("tensor")
    dp = lax.axis_index("dp")
    mz = dp // 8
    my = lax.rem(dp // 2, 4)
    mc = lax.rem(dp, 2)
    right = lax.rem(me + 1, NX)
    left = lax.rem(me + 3, NX)
    opp = lax.rem(me + 2, NX)
    yp, ym, yo = lax.rem(my + 1, 4), lax.rem(my + 3, 4), lax.rem(my + 2, 4)
    zp, zm, zo = lax.rem(mz + 1, 4), lax.rem(mz + 3, 4), lax.rem(mz + 2, 4)

    def dpi(z, y, c):
        return {"dp": (z * 4 + y) * 2 + c}

    def rc(src, dst, s, r, dev):
        return pltpu.make_async_remote_copy(
            src_ref=src, dst_ref=dst, send_sem=s, recv_sem=r, device_id=dev, device_id_type=MESH
        )

    loads = [
        (tok_h, tok), (quant_h, quant), (canvas_h, canv), (lift_h, lift), (loc_h, loc),
        (fac_h, fac), (wo_h, woin), (wd_h, wdin), (kc_h, kc), (vc_h, vc), (fin_h, fin),
        (voc_h, voc), (kron_h, kron),
    ]

    def load(k):
        return pltpu.make_async_copy(loads[k][0], loads[k][1], load_sem.at[k])

    own_q = pltpu.make_async_copy(qkv_h, wq.at[mz, my, mc], own_sem.at[0])
    own_u = pltpu.make_async_copy(up_h, wu.at[mz, my, mc], own_sem.at[1])
    own_q.start()
    for k in (6, 7, 0, 1, 12, 2, 3, 4, 5):
        load(k).start()
    own_u.start()
    for k in (8, 9, 10, 11):
        load(k).start()

    barrier = pltpu.get_barrier_semaphore()
    peers = [{"tensor": right}, {"tensor": left}, {"tensor": opp}]
    peers += [dpi(mz, yp, mc), dpi(mz, ym, mc), dpi(zp, my, mc), dpi(zm, my, mc), dpi(mz, my, 1 - mc)]
    for dev in peers:
        pl.semaphore_signal(barrier, inc=1, device_id=dev, device_id_type=MESH)
    pl.semaphore_wait(barrier, len(peers))

    weights = (wq, wo, wu, wd)

    def unit_copies(r, v):
        w = weights[r]
        c0, c1, ch = SPLITS[r][v]
        u = 2 * r + v
        a, ap, am, ao = (my, yp, ym, yo) if v == 0 else (mz, zp, zm, zo)
        b, bp, bm, bo = (mz, zp, zm, zo) if v == 0 else (my, yp, ym, yo)

        def at(ai, bi, lo, hi):
            cols = pl.ds(lo, hi - lo)
            return w.at[bi, ai, mc, :, cols] if v == 0 else w.at[ai, bi, mc, :, cols]

        def dev(ai, bi):
            return dpi(bi, ai, mc) if v == 0 else dpi(ai, bi, mc)

        def copy(k, src, to):
            return rc(src, src, us.at[u, k], ur.at[u, k], to)

        send = [
            lambda: copy(0, at(a, b, c0, c1), dev(ap, b)),
            lambda: copy(1, at(a, b, c0, c1), dev(am, b)),
            lambda: copy(2, at(am, b, c0, ch), dev(ap, b)),
            lambda: copy(3, at(ap, b, ch, c1), dev(am, b)),
            lambda: copy(4, at(slice(None), b, c0, c1), dev(a, bp)),
            lambda: copy(5, at(slice(None), b, c0, c1), dev(a, bm)),
            lambda: copy(6, at(pl.ds(0, 2), bm, c0, c1), dev(a, bp)),
            lambda: copy(7, at(pl.ds(2, 2), bp, c0, c1), dev(a, bm)),
            lambda: copy(8, w.at[:, :, mc, :, pl.ds(c0, c1 - c0)], dpi(mz, my, 1 - mc)),
        ]
        recv = [
            lambda: copy(0, at(am, b, c0, c1), dev(ap, b)),
            lambda: copy(1, at(ap, b, c0, c1), dev(am, b)),
            lambda: copy(2, at(ao, b, c0, ch), dev(ap, b)),
            lambda: copy(3, at(ao, b, ch, c1), dev(am, b)),
            lambda: copy(4, at(slice(None), bm, c0, c1), dev(a, bp)),
            lambda: copy(5, at(slice(None), bp, c0, c1), dev(a, bm)),
            lambda: copy(6, at(pl.ds(0, 2), bo, c0, c1), dev(a, bp)),
            lambda: copy(7, at(pl.ds(2, 2), bo, c0, c1), dev(a, bm)),
            lambda: copy(8, w.at[:, :, 1 - mc, :, pl.ds(c0, c1 - c0)], dpi(mz, my, 1 - mc)),
        ]
        return send, recv

    def step(r, k):
        for i in (0, 1):
            for v in (0, 1):
                send, recv = unit_copies(r, v)
                if k == 1:
                    send[i]().start()
                elif k in (2, 4):
                    recv[2 * k - 4 + i]().wait_recv()
                    send[2 * k - 2 + i]().start()
                elif k in (3, 5):
                    if i == 0:
                        recv[2 * k - 4]().wait_recv()
                        recv[2 * k - 3]().wait_recv()
                        if k == 5:
                            send[8]().start()
                    if k == 3:
                        send[4 + i]().start()
                elif k == 6 and i == 0:
                    recv[8]().wait_recv()

    own_q.wait()
    step(0, 1)

    load(6).wait()
    load(7).wait()
    eye = (
        lax.broadcasted_iota(jnp.int32, (SH, SH), 0) == lax.broadcasted_iota(jnp.int32, (SH, SH), 1)
    ).astype(BF)
    mycols = pl.ds(pl.multiple_of(me * LW, 128), LW)
    wo[mz, my, mc, :, mycols] = dot_nt(eye, woin[...]).astype(BF)
    for n in range(3):
        wd[mz, my, mc, :, n * 512 : (n + 1) * 512] = dot_nt(
            eye, wdin[n * 512 : (n + 1) * 512, :]
        ).astype(BF)

    def wo_copy(k, owner, to):
        part = wo.at[mz, my, mc, :, pl.ds(pl.multiple_of(owner * LW, 128), LW)]
        return rc(part, part, wos.at[k], wor.at[k], {"tensor": to})

    wo_sends = [wo_copy(0, me, right), wo_copy(1, me, left), wo_copy(2, me, opp)]
    wo_recvs = [wo_copy(0, left, right), wo_copy(1, right, left), wo_copy(2, opp, opp)]
    for c in wo_sends:
        c.start()

    load(0).wait()
    load(1).wait()
    emb[...] = jnp.zeros_like(emb)

    def embed(n, carry):
        base = pl.multiple_of(n * 512, 512)
        ids = lax.broadcasted_iota(jnp.int32, (IMGS * PREVPAD, 512), 1) + base
        onehot = jnp.where(tok[...] == ids, 1.0, 0.0).astype(BF)
        emb[...] += dot(onehot, quant[pl.ds(base, 512), :].astype(BF))
        return carry

    lax.fori_loop(0, 4, embed, 0)
    step(0, 2)
    lax.fori_loop(4, 8, embed, 0)

    def modulated(rows_value, scale, shift):
        center = rows_value - jnp.mean(rows_value, axis=-1, keepdims=True)
        variance = jnp.mean(center * center, axis=-1, keepdims=True)
        return (center * lax.rsqrt(variance + FLOOR) * (1.0 + scale) + shift).astype(BF)

    for k in (12, 2, 3, 4, 5):
        load(k).wait()

    ORDER = (2, 1, 3, 0)

    def first_norm(jj, carry):
        j = lax.rem(me + pick(jj, ORDER), NX)
        rows = emb[pl.ds(pl.multiple_of(j * PREVPAD, 16), PREVPAD), :]
        lifted = lax.dot_general(
            kron[...], rows, (((1,), (0,)), ((), ())),
            precision=lax.Precision.HIGHEST, preferred_element_type=F32,
        )
        can = canv[j] + lifted
        cout[j] = can
        canb = can.astype(BF)
        for n in range(3):
            cols = slice(n * 512, (n + 1) * 512)
            st[:, cols] = dot(canb, lift[:, cols].astype(BF)) + loc[:, cols]
        scale = fac[j, 2:3, :]
        shift = fac[j, 4:5, :]

        def rows_norm(m, c):
            r = pl.ds(pl.multiple_of(m * 64, 64), 64)
            nb1[j, r, :] = modulated(st[r, :], scale, shift)
            return c

        lax.fori_loop(0, 4, rows_norm, 0)

        @pl.when(jj == 0)
        def _():
            step(0, 3)
            for c in wo_recvs:
                c.wait_recv()
            step(1, 1)

        return carry

    lax.fori_loop(0, 3, first_norm, 0)
    step(0, 4)
    step(1, 2)
    lax.fori_loop(3, 4, first_norm, 0)
    out_canvas = pltpu.make_async_copy(cout, canvas_o, cout_sem.at[0])
    out_canvas.start()

    load(8).wait()
    load(9).wait()

    def to_head(lanes):
        return (
            (lanes >= HDIM).astype(jnp.int32)
            + (lanes >= 2 * HDIM).astype(jnp.int32)
            + (lanes >= 3 * HDIM).astype(jnp.int32)
        )

    block_ones = jnp.where(to_head(lax.broadcasted_iota(jnp.int32, (LW, LW), 0))
        == to_head(lax.broadcasted_iota(jnp.int32, (LW, LW), 1)), 1.0, 0.0).astype(BF)
    lane_row = to_head(lax.broadcasted_iota(jnp.int32, (1, LW), 1))
    sharp = jnp.where(
        lane_row == 0,
        sharp_s[0, 0],
        jnp.where(lane_row == 1, sharp_s[0, 1], jnp.where(lane_row == 2, sharp_s[0, 2], sharp_s[0, 3])),
    )

    def unit(u):
        return u * lax.rsqrt(dot((u * u).astype(BF), block_ones) + 1.0)

    def cache_keys(j, carry):
        knc[j] = unit(kc[j].astype(F32)).astype(BF)
        return carry

    lax.fori_loop(0, 2, cache_keys, 0)
    step(0, 5)
    step(1, 3)
    own_u.wait()
    step(2, 1)
    lax.fori_loop(2, 4, cache_keys, 0)
    step(0, 6)

    def att_copy(jj, owner, to):
        return rc(att.at[jj], attr.at[owner], ats.at[jj], atr.at[jj], {"tensor": to})

    def attend(jj, carry):
        off = pick(jj, ORDER)
        j = lax.rem(me + off, NX)
        x = nb1[j]
        q = dot(x, wq[:, :, :, :, 0:LW].reshape(D, LW))
        qn[...] = (unit(q) * sharp).astype(BF)
        k = dot(x, wq[:, :, :, :, LW : 2 * LW].reshape(D, LW))
        kn[...] = unit(k).astype(BF)
        vn[...] = dot(x, wq[:, :, :, :, 2 * LW : 3 * LW].reshape(D, LW)).astype(BF)
        for h in range(HEADS_L):
            w0, w1 = WINDOWS[h]
            lanes = lax.broadcasted_iota(jnp.int32, (TOK, w1 - w0), 1) + w0
            mine = (lanes >= h * HDIM) & (lanes < (h + 1) * HDIM)
            qh = jnp.where(mine, qn[:, w0:w1], jnp.zeros((), BF))
            sc = dot_nt(qh, knc[j, :, w0:w1])
            sn = dot_nt(qh, kn[:, w0:w1])
            top = jnp.maximum(
                jnp.max(sc, axis=-1, keepdims=True), jnp.max(sn, axis=-1, keepdims=True)
            )
            pc = jnp.exp(sc - top)
            pn = jnp.exp(sn - top)
            total = jnp.sum(pc, axis=-1, keepdims=True) + jnp.sum(pn, axis=-1, keepdims=True)
            o = dot(pc.astype(BF), vc[j, :, w0:w1]) + dot(pn.astype(BF), vn[:, w0:w1])
            o = (o * (1.0 / total)).astype(BF)
            if h == 0:
                att[jj, :, w0:w1] = o
            else:
                att[jj, :, w0:w1] = jnp.where(mine, o, att[jj, :, w0:w1])

        @pl.when(jj == 0)
        def _():
            step(2, 2)
            step(1, 4)

        @pl.when(jj == 1)
        def _():
            step(2, 3)
            step(1, 5)
            step(3, 1)

        @pl.when(jj == 2)
        def _():
            step(3, 2)
            step(2, 4)

        @pl.when(jj < 3)
        def _():
            att_copy(jj, me, j).start()

        return carry

    att[...] = jnp.zeros_like(att)
    lax.fori_loop(0, 4, attend, 0)
    attr[me] = att[3]
    step(3, 3)
    step(2, 5)
    step(1, 6)
    for jj in range(3):
        att_copy(jj, lax.rem(me + 4 - ORDER[jj], NX), opp).wait_recv()

    def mix(z, carry):
        cols = pl.ds(pl.multiple_of(z * LW, 128), LW)
        mixed = jnp.zeros((TOK, LW), F32)
        for g in range(NX):
            w = wo[z, :, :, :, g * LW : (g + 1) * LW].reshape(LW, LW)
            mixed = mixed + dot_nt(attr[g], w).astype(BF).astype(F32)
        st[:, cols] = st[:, cols] + fac[me, 0:1, cols] * mixed
        return carry

    lax.fori_loop(0, 4, mix, 0)

    scale2 = fac[me, 3:4, :]
    shift2 = fac[me, 5:6, :]

    def second_norm(m, c):
        r = pl.ds(pl.multiple_of(m * 64, 64), 64)
        nb2[me, r, :] = modulated(st[r, :], scale2, shift2)
        return c

    lax.fori_loop(0, 4, second_norm, 0)

    H = (pl.ds(0, HALF), pl.ds(HALF, HALF))

    def gather_copies(nb, ss, rs):
        def c(k, img, half, to):
            ref = nb.at[img, H[half], :]
            return rc(ref, ref, ss.at[k], rs.at[k], {"tensor": to})

        send = [
            c(0, me, 0, right), c(1, me, 1, left), c(2, me, 1, right), c(3, me, 0, left),
            c(4, left, 0, right), c(5, right, 1, left),
        ]
        recv = [
            c(0, left, 0, right), c(1, right, 1, left), c(2, left, 1, right), c(3, right, 0, left),
            c(4, opp, 0, right), c(5, opp, 1, left),
        ]
        return send, recv

    def gather_steps(s, send, recv):
        @pl.when(s == 1)
        def _():
            recv[0].wait_recv()
            send[4].start()
            recv[1].wait_recv()
            send[5].start()

        @pl.when(s == 2)
        def _():
            recv[2].wait_recv()
            recv[3].wait_recv()

        @pl.when(s == 3)
        def _():
            recv[4].wait_recv()
            recv[5].wait_recv()

    def blocks(s):
        ia = lax.rem(me + pick(s, (0, 3, 3, 2)), NX)
        ib = lax.rem(me + pick(s, (0, 1, 1, 2)), NX)
        ha = pick(s, (0, 0, 1, 0))
        hb = pick(s, (1, 1, 0, 1))
        ra = pl.ds(pl.multiple_of(ha * HALF, HALF), HALF)
        rb = pl.ds(pl.multiple_of(hb * HALF, HALF), HALF)
        return ia, ra, ib, rb

    send2, recv2 = gather_copies(nb2, g2s, g2r)
    for k in range(4):
        send2[k].start()
    step(3, 4)
    step(2, 6)

    def part_copy(s, k, img, src_img, dst_rows):
        i = (s - 1) * 2 + k
        return rc(
            pbuf.at[s, H[k], :], precv.at[src_img, dst_rows, :], rss.at[i], rsr.at[i], {"tensor": img}
        )

    def feed_forward(s, carry):
        gather_steps(s, send2, recv2)
        ia, ra, ib, rb = blocks(s)

        def widen(n, c):
            cols = pl.ds(pl.multiple_of(n * LW, 128), LW)
            x = jnp.concatenate([nb2[ia, ra, :], nb2[ib, rb, :]], axis=0)
            u = dot(x, wu[:, :, :, :, cols].reshape(D, LW))
            act = 0.5 * u * (1.0 + jnp.tanh(0.7978845608028654 * (u + 0.044715 * (u * u * u))))
            hid[:, cols] = act.astype(BF)
            return c

        lax.fori_loop(0, 4, widen, 0)

        @pl.when(s == 0)
        def _():
            step(3, 5)
            step(3, 6)

        def narrow(z, c):
            cols = pl.ds(pl.multiple_of(z * LW, 128), LW)
            pbuf[s, :, cols] = dot_nt(hid[...], wd[z].reshape(LW, D)).astype(BF)
            return c

        lax.fori_loop(0, 4, narrow, 0)

        @pl.when(s >= 1)
        def _():
            part_copy(s, 0, ia, me, ra).start()
            part_copy(s, 1, ib, me, rb).start()

        return carry

    lax.fori_loop(0, 4, feed_forward, 0)

    part_recvs = [
        (1, 0, right, 0), (1, 1, left, 1), (2, 0, right, 1), (2, 1, left, 0), (3, 0, opp, 0), (3, 1, opp, 1),
    ]
    for s, k, src, half in part_recvs:
        part_copy(s, k, src, src, H[half]).wait_recv()
    load(10).wait()
    load(11).wait()

    gamma2 = fac[me, 1:2, :]
    scale3 = fin[me, 0:1, :]
    shift3 = fin[me, 1:2, :]

    def third_norm(m, c):
        r = pl.ds(pl.multiple_of(m * 64, 64), 64)
        mixed = pbuf[0, r, :].astype(F32) + precv[left, r, :].astype(F32)
        mixed = mixed + precv[right, r, :].astype(F32) + precv[opp, r, :].astype(F32)
        nb3[me, r, :] = modulated(st[r, :] + gamma2 * mixed, scale3, shift3)
        return c

    lax.fori_loop(0, 4, third_norm, 0)

    send3, recv3 = gather_copies(nb3, g3s, g3r)
    for k in range(4):
        send3[k].start()

    def out_copy(s, k, img, rows):
        return pltpu.make_async_copy(
            lout.at[s, H[k], :], logits_h.at[img, rows, :], out_sem.at[2 * s + k]
        )

    def head(s, carry):
        gather_steps(s, send3, recv3)
        ia, ra, ib, rb = blocks(s)

        def tile(n, c):
            cols = pl.ds(pl.multiple_of(n * 256, 256), 256)
            x = jnp.concatenate([nb3[ia, ra, :], nb3[ib, rb, :]], axis=0)
            lout[s, :, cols] = dot(x, voc[:, cols]).astype(BF)
            return c

        lax.fori_loop(0, 4, tile, 0)
        out_copy(s, 0, ia, ra).start()
        out_copy(s, 1, ib, rb).start()
        return carry

    lax.fori_loop(0, 4, head, 0)

    for r in range(4):
        for v in (0, 1):
            send, _ = unit_copies(r, v)
            for k in range(9):
                send[k]().wait_send()
    for c in wo_sends:
        c.wait_send()
    for jj in range(3):
        att_copy(jj, me, opp).wait_send()
    for k in range(6):
        send2[k].wait_send()
        send3[k].wait_send()
    for s, k, src, half in part_recvs:
        part_copy(s, k, src, src, H[half]).wait_send()
    out_canvas.wait()

    def out_done(s, carry):
        ia, ra, ib, rb = blocks(s)
        out_copy(s, 0, ia, ra).wait()
        out_copy(s, 1, ib, rb).wait()
        return carry

    lax.fori_loop(0, 4, out_done, 0)


def local(
    sampled_earlier_tokens,
    quantizer_vectors,
    summed_latent_canvas,
    latent_lift_matrix,
    location_tier_offset,
    adaptive_norm_factors,
    logit_sharpness,
    probe_match_content_matrix,
    mixing_projection_matrix,
    widening_projection_matrix,
    narrowing_projection_matrix,
    cached_lower_grid_lookups,
    cached_lower_grid_payloads,
    final_norm_factors,
    vocabulary_logit_matrix,
):
    tokens = jnp.pad(sampled_earlier_tokens, ((0, 0), (0, PREVPAD - PREV * PREV)), constant_values=-1)
    tokens = tokens.reshape(IMGS * PREVPAD, 1)
    operands = (
        tokens,
        quantizer_vectors,
        summed_latent_canvas,
        latent_lift_matrix,
        location_tier_offset,
        adaptive_norm_factors[0],
        logit_sharpness,
        probe_match_content_matrix[0].reshape(SH, 3 * LW),
        mixing_projection_matrix[0],
        widening_projection_matrix[0],
        narrowing_projection_matrix[0],
        cached_lower_grid_lookups[0],
        cached_lower_grid_payloads[0],
        final_norm_factors,
        vocabulary_logit_matrix,
        jnp.asarray(upsample_matrix()),
    )
    anyspace = pl.BlockSpec(memory_space=pl.ANY)
    specs = [anyspace] * len(operands)
    specs[6] = pl.BlockSpec(memory_space=pltpu.SMEM)
    vm = pltpu.VMEM
    dma = pltpu.SemaphoreType.DMA
    scratch = [
        vm((IMGS * PREVPAD, 1), jnp.int32),
        vm((VOCAB, CVAE), F32),
        vm((IMGS, TOK, CVAE), F32),
        vm((CVAE, D), F32),
        vm((TOK, D), F32),
        vm((IMGS, 6, D), F32),
        vm((LW, SH), BF),
        vm((D, SH), BF),
        vm((IMGS, CACHE, LW), BF),
        vm((IMGS, CACHE, LW), BF),
        vm((IMGS, 2, D), F32),
        vm((D, VL), BF),
        vm((TOK, PREVPAD), F32),
        vm((4, 4, 2, SH, 3 * LW), BF),
        vm((4, 4, 2, SH, D), BF),
        vm((4, 4, 2, SH, D), BF),
        vm((4, 4, 2, SH, D), BF),
        vm((IMGS * PREVPAD, CVAE), F32),
        vm((IMGS, TOK, CVAE), F32),
        vm((TOK, D), F32),
        vm((IMGS, TOK, D), BF),
        vm((IMGS, TOK, D), BF),
        vm((IMGS, TOK, D), BF),
        vm((TOK, LW), BF),
        vm((TOK, LW), BF),
        vm((TOK, LW), BF),
        vm((IMGS, CACHE, LW), BF),
        vm((NX, TOK, LW), BF),
        vm((NX, TOK, LW), BF),
        vm((TOK, D), BF),
        vm((NX, TOK, D), BF),
        vm((NX, TOK, D), BF),
        vm((NX, TOK, VL), BF),
        dma((13,)), dma((2,)), dma((8,)), dma((1,)),
        dma((8, 9)), dma((8, 9)), dma((3,)), dma((3,)), dma((3,)), dma((3,)),
        dma((6,)), dma((6,)), dma((6,)), dma((6,)), dma((6,)), dma((6,)),
    ]
    return pl.pallas_call(
        body,
        out_shape=(
            jax.ShapeDtypeStruct((IMGS, TOK, VL), BF),
            jax.ShapeDtypeStruct((IMGS, TOK, CVAE), F32),
        ),
        in_specs=specs,
        out_specs=(anyspace, anyspace),
        scratch_shapes=scratch,
        compiler_params=pltpu.CompilerParams(
            collective_id=0, has_side_effects=True, vmem_limit_bytes=67_000_000
        ),
    )(*operands)


def solution(mesh):
    placed = (
        P("dp", None),
        P(),
        P("dp", None, None),
        P(),
        P(),
        P(None, "dp", None, None),
        P(None, "tensor"),
        P(None, "dp", None, "tensor"),
        P(None, "tensor", "dp"),
        P(None, "dp", "tensor"),
        P(None, "tensor", "dp"),
        P(None, "dp", None, "tensor"),
        P(None, "dp", None, "tensor"),
        P("dp", None, None),
        P(None, "tensor"),
    )
    return jax.shard_map(
        local,
        mesh=mesh,
        in_specs=placed,
        out_specs=(P("dp", None, "tensor"), P("dp", None, None)),
        check_vma=False,
    )
```

```python
import numpy as np
import jax
import jax.numpy as jnp
from jax import lax
from jax.experimental import pallas as pl
from jax.experimental.pallas import tpu as pltpu
from jax.sharding import PartitionSpec as P

MESH = pl.DeviceIdType.MESH
BF = jnp.bfloat16
F32 = jnp.float32

D = 1536
HEADS_L = 4
HDIM = 96
LW = HEADS_L * HDIM
VOCAB = 4096
VL = 1024
CVAE = 32
SIDE = 16
PREV = 13
PREVTOK = 169
CACHE = 424
TOK = 256
HALF = 128
IMGS = 4
SH = 48
NX = 4
FLOOR = 0.1

WINDOWS = ((0, 128), (0, 256), (128, 384), (256, 384))

SPLITS = (
    ((0, 640, 384), (640, 1152, 896)),
    ((0, 768, 384), (768, 1536, 1152)),
    ((0, 768, 384), (768, 1536, 1152)),
    ((0, 768, 384), (768, 1536, 1152)),
)


def upsample_matrix():
    a = np.arange(SIDE)
    num = np.maximum((2 * a + 1) * PREV - SIDE, 0)
    low = num // (2 * SIDE)
    frac = (num % (2 * SIDE)) / (2.0 * SIDE)
    up = np.zeros((SIDE, PREV))
    up[a, low] += 1.0 - frac
    up[a, np.minimum(low + 1, PREV - 1)] += frac
    return np.kron(up, up).T.astype(np.float32)


def dot(a, b):
    return jnp.dot(a, b, preferred_element_type=F32)


def dot_nt(a, b):
    return lax.dot_general(a, b, (((1,), (1,)), ((), ())), preferred_element_type=F32)


def pick(index, values):
    out = values[-1]
    for k in range(len(values) - 1):
        out = jnp.where(index == k, values[k], out)
    return out


def body(
    tok_h, quant_h, canvas_h, lift_h, loc_h, fac_h, sharp_s, qkv_h, wo_h, up_h, wd_h,
    kc_h, vc_h, fin_h, voc_h, kron_h,
    logits_h, canvas_o,
    tok, quant, canv, lift, loc, fac, kc, vc, fin, voc, kron,
    wq, wo, wu, wd,
    emb, cout, st, nb1, nb2, nb3, qn, kn, vn, knc, att, attr, hid, pbuf, precv, lout,
    load_sem, own_sem, out_sem, cout_sem,
    us, ur, wos, wor, ats, atr, g2s, g2r, rss, rsr, g3s, g3r,
):
    me = lax.axis_index("tensor")
    dp = lax.axis_index("dp")
    mz = dp // 8
    my = lax.rem(dp // 2, 4)
    mc = lax.rem(dp, 2)
    right = lax.rem(me + 1, NX)
    left = lax.rem(me + 3, NX)
    opp = lax.rem(me + 2, NX)
    yp, ym, yo = lax.rem(my + 1, 4), lax.rem(my + 3, 4), lax.rem(my + 2, 4)
    zp, zm, zo = lax.rem(mz + 1, 4), lax.rem(mz + 3, 4), lax.rem(mz + 2, 4)

    def dpi(z, y, c):
        return {"dp": (z * 4 + y) * 2 + c}

    def rc(src, dst, s, r, dev):
        return pltpu.make_async_remote_copy(
            src_ref=src, dst_ref=dst, send_sem=s, recv_sem=r, device_id=dev, device_id_type=MESH
        )

    mycols = pl.ds(pl.multiple_of(me * LW, 128), LW)
    loads = [
        (tok_h, tok), (quant_h, quant), (canvas_h, canv), (lift_h, lift), (loc_h, loc),
        (fac_h, fac), (wo_h, wo.at[mz, my, mc, :, mycols]), (wd_h, wd.at[mz, my, mc]),
        (kc_h, kc), (vc_h, vc), (fin_h, fin), (voc_h, voc), (kron_h, kron),
    ]

    def load(k):
        return pltpu.make_async_copy(loads[k][0], loads[k][1], load_sem.at[k])

    own_q = [
        pltpu.make_async_copy(
            qkv_h.at[k], wq.at[mz, my, mc, :, pl.ds(k * LW, LW)], own_sem.at[1 + k]
        )
        for k in range(3)
    ]
    own_u = pltpu.make_async_copy(up_h, wu.at[mz, my, mc], own_sem.at[0])
    for c in own_q:
        c.start()
    for k in (6, 7, 0, 1, 12, 2, 3, 4, 5):
        load(k).start()
    own_u.start()
    for k in (8, 9, 10, 11):
        load(k).start()

    barrier = pltpu.get_barrier_semaphore()
    peers = [{"tensor": right}, {"tensor": left}, {"tensor": opp}]
    peers += [dpi(mz, yp, mc), dpi(mz, ym, mc), dpi(zp, my, mc), dpi(zm, my, mc), dpi(mz, my, 1 - mc)]
    for dev in peers:
        pl.semaphore_signal(barrier, inc=1, device_id=dev, device_id_type=MESH)
    pl.semaphore_wait(barrier, len(peers))

    weights = (wq, wo, wu, wd)

    def unit_copies(r, v):
        w = weights[r]
        c0, c1, ch = SPLITS[r][v]
        u = 2 * r + v
        a, ap, am, ao = (my, yp, ym, yo) if v == 0 else (mz, zp, zm, zo)
        b, bp, bm, bo = (mz, zp, zm, zo) if v == 0 else (my, yp, ym, yo)

        def at(ai, bi, lo, hi):
            cols = pl.ds(lo, hi - lo)
            return w.at[bi, ai, mc, :, cols] if v == 0 else w.at[ai, bi, mc, :, cols]

        def dev(ai, bi):
            return dpi(bi, ai, mc) if v == 0 else dpi(ai, bi, mc)

        def copy(k, src, to):
            return rc(src, src, us.at[u, k], ur.at[u, k], to)

        send = [
            lambda: copy(0, at(a, b, c0, c1), dev(ap, b)),
            lambda: copy(1, at(a, b, c0, c1), dev(am, b)),
            lambda: copy(2, at(am, b, c0, ch), dev(ap, b)),
            lambda: copy(3, at(ap, b, ch, c1), dev(am, b)),
            lambda: copy(4, at(slice(None), b, c0, c1), dev(a, bp)),
            lambda: copy(5, at(slice(None), b, c0, c1), dev(a, bm)),
            lambda: copy(6, at(pl.ds(0, 2), bm, c0, c1), dev(a, bp)),
            lambda: copy(7, at(pl.ds(2, 2), bp, c0, c1), dev(a, bm)),
            lambda: copy(8, w.at[:, :, mc, :, pl.ds(c0, c1 - c0)], dpi(mz, my, 1 - mc)),
        ]
        recv = [
            lambda: copy(0, at(am, b, c0, c1), dev(ap, b)),
            lambda: copy(1, at(ap, b, c0, c1), dev(am, b)),
            lambda: copy(2, at(ao, b, c0, ch), dev(ap, b)),
            lambda: copy(3, at(ao, b, ch, c1), dev(am, b)),
            lambda: copy(4, at(slice(None), bm, c0, c1), dev(a, bp)),
            lambda: copy(5, at(slice(None), bp, c0, c1), dev(a, bm)),
            lambda: copy(6, at(pl.ds(0, 2), bo, c0, c1), dev(a, bp)),
            lambda: copy(7, at(pl.ds(2, 2), bo, c0, c1), dev(a, bm)),
            lambda: copy(8, w.at[:, :, 1 - mc, :, pl.ds(c0, c1 - c0)], dpi(mz, my, 1 - mc)),
        ]
        return send, recv

    def step(r, k):
        for i in (0, 1):
            for v in (0, 1):
                send, recv = unit_copies(r, v)
                if k == 1:
                    send[i]().start()
                elif k in (2, 4):
                    recv[2 * k - 4 + i]().wait_recv()
                    send[2 * k - 2 + i]().start()
                elif k in (3, 5):
                    if i == 0:
                        recv[2 * k - 4]().wait_recv()
                        recv[2 * k - 3]().wait_recv()
                        if k == 5:
                            send[8]().start()
                    if k == 3:
                        send[4 + i]().start()
                elif k == 6 and i == 0:
                    recv[8]().wait_recv()

    for c in own_q:
        c.wait()
    step(0, 1)

    load(6).wait()
    load(7).wait()

    def wo_copy(k, owner, to):
        part = wo.at[mz, my, mc, :, pl.ds(pl.multiple_of(owner * LW, 128), LW)]
        return rc(part, part, wos.at[k], wor.at[k], {"tensor": to})

    wo_sends = [wo_copy(0, me, right), wo_copy(1, me, left), wo_copy(2, me, opp)]
    wo_recvs = [wo_copy(0, left, right), wo_copy(1, right, left), wo_copy(2, opp, opp)]
    for c in wo_sends:
        c.start()

    load(0).wait()
    load(1).wait()
    emb[...] = jnp.zeros_like(emb)

    def high_low(v):
        high = v.astype(BF)
        return high, (v - high.astype(F32)).astype(BF)

    def embed(n, carry):
        base = pl.multiple_of(n * 512, 512)
        table = jnp.concatenate(high_low(quant[:, pl.ds(base, 512)]), axis=0)
        ids = lax.broadcasted_iota(jnp.int32, (512, PREVTOK), 0) + base
        for j in range(IMGS):
            onehot = jnp.where(tok[j : j + 1, :] == ids, 1.0, 0.0).astype(BF)
            emb[j] += dot(table, onehot)
        return carry

    lax.fori_loop(0, 4, embed, 0)
    step(0, 2)
    lax.fori_loop(4, 8, embed, 0)

    def modulated(rows_value, scale, shift):
        center = rows_value - jnp.mean(rows_value, axis=-1, keepdims=True)
        variance = jnp.mean(center * center, axis=-1, keepdims=True)
        return (center * lax.rsqrt(variance + FLOOR) * (1.0 + scale) + shift).astype(BF)

    for k in (12, 2, 3, 4, 5):
        load(k).wait()

    ORDER = (2, 1, 3, 0)

    def first_norm(jj, carry):
        j = lax.rem(me + pick(jj, ORDER), NX)
        rows = emb[j, 0:CVAE, :] + emb[j, CVAE : 2 * CVAE, :]
        lifted = lax.dot_general(
            rows, kron[...], (((1,), (0,)), ((), ())),
            precision=lax.Precision.HIGHEST, preferred_element_type=F32,
        )
        can = canv[j] + lifted
        cout[j] = can
        can_hi, can_lo = high_low(can)
        can3 = jnp.concatenate([can_hi, can_lo, can_hi], axis=0)
        for n in range(3):
            cols = slice(n * 512, (n + 1) * 512)
            lift_hi, lift_lo = high_low(lift[:, cols])
            lift3 = jnp.concatenate([lift_hi, lift_hi, lift_lo], axis=0)
            st[:, cols] = loc[:, cols] + lax.dot_general(
                can3, lift3, (((0,), (0,)), ((), ())), preferred_element_type=F32
            )
        scale = fac[2, pl.ds(j, 1), :]
        shift = fac[4, pl.ds(j, 1), :]

        def rows_norm(m, c):
            r = pl.ds(pl.multiple_of(m * 64, 64), 64)
            nb1[j, r, :] = modulated(st[r, :], scale, shift)
            return c

        lax.fori_loop(0, 4, rows_norm, 0)

        @pl.when(jj == 0)
        def _():
            step(0, 3)
            for c in wo_recvs:
                c.wait_recv()
            step(1, 1)

        return carry

    lax.fori_loop(0, 3, first_norm, 0)
    step(0, 4)
    step(1, 2)
    lax.fori_loop(3, 4, first_norm, 0)
    out_canvas = pltpu.make_async_copy(cout, canvas_o, cout_sem.at[0])
    out_canvas.start()

    load(8).wait()
    load(9).wait()

    def to_head(lanes):
        return (
            (lanes >= HDIM).astype(jnp.int32)
            + (lanes >= 2 * HDIM).astype(jnp.int32)
            + (lanes >= 3 * HDIM).astype(jnp.int32)
        )

    block_ones = jnp.where(to_head(lax.broadcasted_iota(jnp.int32, (LW, LW), 0))
        == to_head(lax.broadcasted_iota(jnp.int32, (LW, LW), 1)), 1.0, 0.0).astype(BF)
    lane_row = to_head(lax.broadcasted_iota(jnp.int32, (1, LW), 1))
    sharp = jnp.where(
        lane_row == 0,
        sharp_s[0, 0],
        jnp.where(lane_row == 1, sharp_s[0, 1], jnp.where(lane_row == 2, sharp_s[0, 2], sharp_s[0, 3])),
    )

    def unit(u):
        return u * lax.rsqrt(dot((u * u).astype(BF), block_ones) + 1.0)

    def cache_keys(j, carry):
        knc[j] = unit(kc[j].astype(F32)).astype(BF)
        return carry

    lax.fori_loop(0, 2, cache_keys, 0)
    step(0, 5)
    step(1, 3)
    own_u.wait()
    step(2, 1)
    lax.fori_loop(2, 4, cache_keys, 0)
    step(0, 6)

    def att_copy(jj, owner, to):
        return rc(att.at[jj], attr.at[owner], ats.at[jj], atr.at[jj], {"tensor": to})

    def attend(jj, carry):
        off = pick(jj, ORDER)
        j = lax.rem(me + off, NX)
        x = nb1[j]
        q = dot(x, wq[:, :, :, :, 0:LW].reshape(D, LW))
        qn[...] = (unit(q) * sharp).astype(BF)
        k = dot(x, wq[:, :, :, :, LW : 2 * LW].reshape(D, LW))
        kn[...] = unit(k).astype(BF)
        vn[...] = dot(x, wq[:, :, :, :, 2 * LW : 3 * LW].reshape(D, LW)).astype(BF)
        for h in range(HEADS_L):
            w0, w1 = WINDOWS[h]
            lanes = lax.broadcasted_iota(jnp.int32, (TOK, w1 - w0), 1) + w0
            mine = (lanes >= h * HDIM) & (lanes < (h + 1) * HDIM)
            qh = jnp.where(mine, qn[:, w0:w1], jnp.zeros((), BF))
            sc = dot_nt(qh, knc[j, :, w0:w1])
            sn = dot_nt(qh, kn[:, w0:w1])
            top = jnp.maximum(
                jnp.max(sc, axis=-1, keepdims=True), jnp.max(sn, axis=-1, keepdims=True)
            )
            pc = jnp.exp(sc - top)
            pn = jnp.exp(sn - top)
            total = jnp.sum(pc, axis=-1, keepdims=True) + jnp.sum(pn, axis=-1, keepdims=True)
            o = dot(pc.astype(BF), vc[j, :, w0:w1]) + dot(pn.astype(BF), vn[:, w0:w1])
            o = (o * (1.0 / total)).astype(BF)
            if h == 0:
                att[jj, :, w0:w1] = o
            else:
                att[jj, :, w0:w1] = jnp.where(mine, o, att[jj, :, w0:w1])

        @pl.when(jj == 0)
        def _():
            step(2, 2)
            step(1, 4)

        @pl.when(jj == 1)
        def _():
            step(2, 3)
            step(1, 5)
            step(3, 1)

        @pl.when(jj == 2)
        def _():
            step(3, 2)
            step(2, 4)

        @pl.when(jj < 3)
        def _():
            att_copy(jj, me, j).start()

        return carry

    att[...] = jnp.zeros_like(att)
    lax.fori_loop(0, 4, attend, 0)
    attr[me] = att[3]
    step(3, 3)
    step(2, 5)
    step(1, 6)
    for jj in range(3):
        att_copy(jj, lax.rem(me + 4 - ORDER[jj], NX), opp).wait_recv()

    def mix(z, carry):
        cols = pl.ds(pl.multiple_of(z * LW, 128), LW)
        mixed = jnp.zeros((TOK, LW), F32)
        for g in range(NX):
            w = wo[z, :, :, :, g * LW : (g + 1) * LW].reshape(LW, LW)
            mixed = mixed + dot_nt(attr[g], w).astype(BF).astype(F32)
        st[:, cols] = st[:, cols] + fac[0, pl.ds(me, 1), cols] * mixed
        return carry

    lax.fori_loop(0, 4, mix, 0)

    scale2 = fac[3, pl.ds(me, 1), :]
    shift2 = fac[5, pl.ds(me, 1), :]

    def second_norm(m, c):
        r = pl.ds(pl.multiple_of(m * 64, 64), 64)
        nb2[me, r, :] = modulated(st[r, :], scale2, shift2)
        return c

    lax.fori_loop(0, 4, second_norm, 0)

    H = (pl.ds(0, HALF), pl.ds(HALF, HALF))

    def gather_copies(nb, ss, rs):
        def c(k, img, half, to):
            ref = nb.at[img, H[half], :]
            return rc(ref, ref, ss.at[k], rs.at[k], {"tensor": to})

        send = [
            c(0, me, 0, right), c(1, me, 1, left), c(2, me, 1, right), c(3, me, 0, left),
            c(4, left, 0, right), c(5, right, 1, left),
        ]
        recv = [
            c(0, left, 0, right), c(1, right, 1, left), c(2, left, 1, right), c(3, right, 0, left),
            c(4, opp, 0, right), c(5, opp, 1, left),
        ]
        return send, recv

    def gather_steps(s, send, recv):
        @pl.when(s == 1)
        def _():
            recv[0].wait_recv()
            send[4].start()
            recv[1].wait_recv()
            send[5].start()

        @pl.when(s == 2)
        def _():
            recv[2].wait_recv()
            recv[3].wait_recv()

        @pl.when(s == 3)
        def _():
            recv[4].wait_recv()
            recv[5].wait_recv()

    def blocks(s):
        ia = lax.rem(me + pick(s, (0, 3, 3, 2)), NX)
        ib = lax.rem(me + pick(s, (0, 1, 1, 2)), NX)
        ha = pick(s, (0, 0, 1, 0))
        hb = pick(s, (1, 1, 0, 1))
        ra = pl.ds(pl.multiple_of(ha * HALF, HALF), HALF)
        rb = pl.ds(pl.multiple_of(hb * HALF, HALF), HALF)
        return ia, ra, ib, rb

    send2, recv2 = gather_copies(nb2, g2s, g2r)
    for k in range(4):
        send2[k].start()
    step(3, 4)
    step(2, 6)

    def part_copy(s, k, img, src_img, dst_rows):
        i = (s - 1) * 2 + k
        return rc(
            pbuf.at[s, H[k], :], precv.at[src_img, dst_rows, :], rss.at[i], rsr.at[i], {"tensor": img}
        )

    def feed_forward(s, carry):
        gather_steps(s, send2, recv2)
        ia, ra, ib, rb = blocks(s)

        def widen(n, c):
            cols = pl.ds(pl.multiple_of(n * LW, 128), LW)
            x = jnp.concatenate([nb2[ia, ra, :], nb2[ib, rb, :]], axis=0)
            u = dot(x, wu[:, :, :, :, cols].reshape(D, LW))
            act = 0.5 * u * (1.0 + jnp.tanh(0.7978845608028654 * (u + 0.044715 * (u * u * u))))
            hid[:, cols] = act.astype(BF)
            return c

        lax.fori_loop(0, 4, widen, 0)

        @pl.when(s == 0)
        def _():
            step(3, 5)
            step(3, 6)

        def narrow(z, c):
            cols = pl.ds(pl.multiple_of(z * LW, 128), LW)
            pbuf[s, :, cols] = dot_nt(hid[...], wd[z].reshape(LW, D)).astype(BF)
            return c

        lax.fori_loop(0, 4, narrow, 0)

        @pl.when(s >= 1)
        def _():
            part_copy(s, 0, ia, me, ra).start()
            part_copy(s, 1, ib, me, rb).start()

        return carry

    lax.fori_loop(0, 4, feed_forward, 0)

    part_recvs = [
        (1, 0, right, 0), (1, 1, left, 1), (2, 0, right, 1), (2, 1, left, 0), (3, 0, opp, 0), (3, 1, opp, 1),
    ]
    for s, k, src, half in part_recvs:
        part_copy(s, k, src, src, H[half]).wait_recv()
    load(10).wait()
    load(11).wait()

    gamma2 = fac[1, pl.ds(me, 1), :]
    scale3 = fin[me, 0:1, :]
    shift3 = fin[me, 1:2, :]

    def third_norm(m, c):
        r = pl.ds(pl.multiple_of(m * 64, 64), 64)
        mixed = pbuf[0, r, :].astype(F32) + precv[left, r, :].astype(F32)
        mixed = mixed + precv[right, r, :].astype(F32) + precv[opp, r, :].astype(F32)
        nb3[me, r, :] = modulated(st[r, :] + gamma2 * mixed, scale3, shift3)
        return c

    lax.fori_loop(0, 4, third_norm, 0)

    send3, recv3 = gather_copies(nb3, g3s, g3r)
    for k in range(4):
        send3[k].start()

    def out_copy(s, k, img, rows):
        return pltpu.make_async_copy(
            lout.at[s, H[k], :], logits_h.at[img, rows, :], out_sem.at[2 * s + k]
        )

    def head(s, carry):
        gather_steps(s, send3, recv3)
        ia, ra, ib, rb = blocks(s)

        def tile(n, c):
            cols = pl.ds(pl.multiple_of(n * 256, 256), 256)
            x = jnp.concatenate([nb3[ia, ra, :], nb3[ib, rb, :]], axis=0)
            lout[s, :, cols] = dot(x, voc[:, cols]).astype(BF)
            return c

        lax.fori_loop(0, 4, tile, 0)
        out_copy(s, 0, ia, ra).start()
        out_copy(s, 1, ib, rb).start()
        return carry

    lax.fori_loop(0, 4, head, 0)

    for r in range(4):
        for v in (0, 1):
            send, _ = unit_copies(r, v)
            for k in range(9):
                send[k]().wait_send()
    for c in wo_sends:
        c.wait_send()
    for jj in range(3):
        att_copy(jj, me, opp).wait_send()
    for k in range(6):
        send2[k].wait_send()
        send3[k].wait_send()
    for s, k, src, half in part_recvs:
        part_copy(s, k, src, src, H[half]).wait_send()
    out_canvas.wait()

    def out_done(s, carry):
        ia, ra, ib, rb = blocks(s)
        out_copy(s, 0, ia, ra).wait()
        out_copy(s, 1, ib, rb).wait()
        return carry

    lax.fori_loop(0, 4, out_done, 0)


def local(
    sampled_earlier_tokens,
    quantizer_vectors,
    summed_latent_canvas,
    latent_lift_matrix,
    location_tier_offset,
    adaptive_norm_factors,
    logit_sharpness,
    probe_match_content_matrix,
    mixing_projection_matrix,
    widening_projection_matrix,
    narrowing_projection_matrix,
    cached_lower_grid_lookups,
    cached_lower_grid_payloads,
    final_norm_factors,
    vocabulary_logit_matrix,
):
    operands = (
        sampled_earlier_tokens,
        quantizer_vectors.T,
        jnp.swapaxes(summed_latent_canvas, 1, 2),
        latent_lift_matrix,
        location_tier_offset,
        jnp.swapaxes(adaptive_norm_factors[0], 0, 1),
        logit_sharpness,
        jnp.swapaxes(probe_match_content_matrix[0], 0, 1),
        mixing_projection_matrix[0].T,
        widening_projection_matrix[0],
        narrowing_projection_matrix[0].T,
        cached_lower_grid_lookups[0],
        cached_lower_grid_payloads[0],
        final_norm_factors,
        vocabulary_logit_matrix,
        jnp.asarray(upsample_matrix()),
    )
    anyspace = pl.BlockSpec(memory_space=pl.ANY)
    specs = [anyspace] * len(operands)
    specs[6] = pl.BlockSpec(memory_space=pltpu.SMEM)
    vm = pltpu.VMEM
    dma = pltpu.SemaphoreType.DMA
    scratch = [
        vm((IMGS, PREVTOK), jnp.int32),
        vm((CVAE, VOCAB), F32),
        vm((IMGS, CVAE, TOK), F32),
        vm((CVAE, D), F32),
        vm((TOK, D), F32),
        vm((6, IMGS, D), F32),
        vm((IMGS, CACHE, LW), BF),
        vm((IMGS, CACHE, LW), BF),
        vm((IMGS, 2, D), F32),
        vm((D, VL), BF),
        vm((PREVTOK, TOK), F32),
        vm((4, 4, 2, SH, 3 * LW), BF),
        vm((4, 4, 2, SH, D), BF),
        vm((4, 4, 2, SH, D), BF),
        vm((4, 4, 2, SH, D), BF),
        vm((IMGS, 2 * CVAE, PREVTOK), F32),
        vm((IMGS, CVAE, TOK), F32),
        vm((TOK, D), F32),
        vm((IMGS, TOK, D), BF),
        vm((IMGS, TOK, D), BF),
        vm((IMGS, TOK, D), BF),
        vm((TOK, LW), BF),
        vm((TOK, LW), BF),
        vm((TOK, LW), BF),
        vm((IMGS, CACHE, LW), BF),
        vm((NX, TOK, LW), BF),
        vm((NX, TOK, LW), BF),
        vm((TOK, D), BF),
        vm((NX, TOK, D), BF),
        vm((NX, TOK, D), BF),
        vm((NX, TOK, VL), BF),
        dma((13,)), dma((4,)), dma((8,)), dma((1,)),
        dma((8, 9)), dma((8, 9)), dma((3,)), dma((3,)), dma((3,)), dma((3,)),
        dma((6,)), dma((6,)), dma((6,)), dma((6,)), dma((6,)), dma((6,)),
    ]
    logits, canvas = pl.pallas_call(
        body,
        out_shape=(
            jax.ShapeDtypeStruct((IMGS, TOK, VL), BF),
            jax.ShapeDtypeStruct((IMGS, CVAE, TOK), F32),
        ),
        in_specs=specs,
        out_specs=(anyspace, anyspace),
        scratch_shapes=scratch,
        compiler_params=pltpu.CompilerParams(
            collective_id=0, has_side_effects=True, vmem_limit_bytes=67_000_000
        ),
    )(*operands)
    return logits, jnp.swapaxes(canvas, 1, 2)


def solution(mesh):
    placed = (
        P("dp", None),
        P(),
        P("dp", None, None),
        P(),
        P(),
        P(None, "dp", None, None),
        P(None, "tensor"),
        P(None, "dp", None, "tensor"),
        P(None, "tensor", "dp"),
        P(None, "dp", "tensor"),
        P(None, "tensor", "dp"),
        P(None, "dp", None, "tensor"),
        P(None, "dp", None, "tensor"),
        P("dp", None, None),
        P(None, "tensor"),
    )
    return jax.shard_map(
        local,
        mesh=mesh,
        in_specs=placed,
        out_specs=(P("dp", None, "tensor"), P("dp", None, None)),
        check_vma=False,
    )
```

```python
import numpy as np
import jax
import jax.numpy as jnp
from jax import lax
from jax.experimental import pallas as pl
from jax.experimental.pallas import tpu as pltpu
from jax.sharding import PartitionSpec as P

MESH = pl.DeviceIdType.MESH
BF = jnp.bfloat16
F32 = jnp.float32

D = 1536
HEADS_L = 4
HDIM = 96
LW = HEADS_L * HDIM
VOCAB = 4096
VL = 1024
CVAE = 32
SIDE = 16
PREV = 13
PREVTOK = 169
CACHE = 424
TOK = 256
HALF = 128
QUART = 64
IMGS = 4
SH = 48
NX = 4
FLOOR = 0.1

WINDOWS = ((0, 128), (0, 256), (128, 384), (256, 384))

QKV_SPLIT = ((0, 640, 384), (640, 1152, 896))
SPLIT = ((0, 768, 384), (768, 1536, 1152))


def upsample_matrix():
    a = np.arange(SIDE)
    num = np.maximum((2 * a + 1) * PREV - SIDE, 0)
    low = num // (2 * SIDE)
    frac = (num % (2 * SIDE)) / (2.0 * SIDE)
    up = np.zeros((SIDE, PREV))
    up[a, low] += 1.0 - frac
    up[a, np.minimum(low + 1, PREV - 1)] += frac
    return np.kron(up, up).T.astype(np.float32)


def dot(a, b):
    return jnp.dot(a, b, preferred_element_type=F32)


def dot_nt(a, b):
    return lax.dot_general(a, b, (((1,), (1,)), ((), ())), preferred_element_type=F32)


def pick(index, values):
    out = values[-1]
    for k in range(len(values) - 1):
        out = jnp.where(index == k, values[k], out)
    return out


def body(
    tok_h, quant_h, canvas_h, lift_h, loc_h, fac_h, sharp_s, qkv_h, wo_h, up_h, wd_h,
    kc_h, vc_h, fin_h, voc_h, kron_h,
    logits_h, canvas_o,
    tok, quant, canv, lift, loc, fac, kc, vc, fin, voc, kron,
    wq, wo, wu, wd,
    emb, cout, st, nb1, nb2, nb3, qn, kn, vn, knc, att, attr, hid, pbuf, precv, pacc, lout,
    load_sem, own_sem, out_sem, cout_sem,
    qs, qr, us, ur, wos, wor, ats, atr, g2s, g2r, rss, rsr, g3s, g3r,
):
    me = lax.axis_index("tensor")
    dp = lax.axis_index("dp")
    mz = dp // 8
    my = lax.rem(dp // 2, 4)
    mc = lax.rem(dp, 2)
    right = lax.rem(me + 1, NX)
    left = lax.rem(me + 3, NX)
    opp = lax.rem(me + 2, NX)
    yp, ym, yo = lax.rem(my + 1, 4), lax.rem(my + 3, 4), lax.rem(my + 2, 4)
    zp, zm, zo = lax.rem(mz + 1, 4), lax.rem(mz + 3, 4), lax.rem(mz + 2, 4)

    def dpi(z, y, c):
        return {"dp": (z * 4 + y) * 2 + c}

    def rc(src, dst, s, r, dev):
        return pltpu.make_async_remote_copy(
            src_ref=src, dst_ref=dst, send_sem=s, recv_sem=r, device_id=dev, device_id_type=MESH
        )

    mycols = pl.ds(pl.multiple_of(me * LW, 128), LW)
    loads = [
        (tok_h, tok), (quant_h, quant), (canvas_h, canv), (lift_h, lift), (loc_h, loc),
        (fac_h, fac), (wo_h, wo.at[mz, my, mc, :, mycols]), (wd_h, wd.at[mz, my, mc]),
        (kc_h, kc), (vc_h, vc), (fin_h, fin), (voc_h, voc), (kron_h, kron),
    ]

    def load(k):
        return pltpu.make_async_copy(loads[k][0], loads[k][1], load_sem.at[k])

    own_q = [
        pltpu.make_async_copy(
            qkv_h.at[k], wq.at[mz, my, mc, :, pl.ds(k * LW, LW)], own_sem.at[1 + k]
        )
        for k in range(3)
    ]
    own_u = pltpu.make_async_copy(up_h, wu.at[mz, my, mc], own_sem.at[0])
    for c in own_q:
        c.start()
    for k in (6, 7, 0, 1, 12, 2, 3, 4, 5):
        load(k).start()
    own_u.start()
    for k in (8, 9, 10, 11):
        load(k).start()

    barrier = pltpu.get_barrier_semaphore()
    peers = [{"tensor": right}, {"tensor": left}, {"tensor": opp}]
    peers += [dpi(mz, yp, mc), dpi(mz, ym, mc), dpi(zp, my, mc), dpi(zm, my, mc), dpi(mz, my, 1 - mc)]
    for dev in peers:
        pl.semaphore_signal(barrier, inc=1, device_id=dev, device_id_type=MESH)
    pl.semaphore_wait(barrier, len(peers))

    weights = (wo, wu, wd)

    def ring(w, split, v, sends, recvs):
        c0, c1, ch = split[v]
        a, ap, am, ao = (my, yp, ym, yo) if v == 0 else (mz, zp, zm, zo)
        b, bp, bm, bo = (mz, zp, zm, zo) if v == 0 else (my, yp, ym, yo)

        def at(ai, bi, lo, hi, core=mc):
            cols = pl.ds(lo, hi - lo)
            return w.at[bi, ai, core, :, cols] if v == 0 else w.at[ai, bi, core, :, cols]

        def dev(ai, bi):
            return dpi(bi, ai, mc) if v == 0 else dpi(ai, bi, mc)

        def copy(k, src, to):
            return rc(src, src, sends.at[k], recvs.at[k], to)

        return c0, c1, ch, (a, ap, am, ao), (b, bp, bm, bo), at, dev, copy

    other = dpi(mz, my, 1 - mc)

    def qkv_copies(v):
        c0, c1, ch, (a, ap, am, ao), (b, bp, bm, bo), at, dev, copy = ring(
            wq, QKV_SPLIT, v, qs.at[v], qr.at[v]
        )
        every = slice(None)
        row = (a, am, ap, ao)
        send = [
            (at(a, b, c0, c1), dev(ap, b)),
            (at(a, b, c0, c1), dev(am, b)),
            (at(am, b, c0, ch), dev(ap, b)),
            (at(ap, b, ch, c1), dev(am, b)),
        ]
        recv = [at(am, b, c0, c1), at(ap, b, c0, c1), at(ao, b, c0, ch), at(ao, b, ch, c1)]
        send += [(at(ai, b, c0, c1), dev(a, bp)) for ai in row]
        recv += [at(ai, bm, c0, c1) for ai in row]
        send += [(at(ai, b, c0, c1), dev(a, bm)) for ai in row]
        recv += [at(ai, bp, c0, c1) for ai in row]
        send += [(at(ai, bm, c0, c1), dev(a, bp)) for ai in row[:2]]
        send += [(at(ai, bp, c0, c1), dev(a, bm)) for ai in row[2:]]
        recv += [at(ai, bo, c0, c1) for ai in row]
        send += [(at(every, bi, c0, c1), other) for bi in (b, bm, bp, bo)]
        recv += [at(every, bi, c0, c1, 1 - mc) for bi in (b, bm, bp, bo)]
        return (
            [lambda k=k, x=x: copy(k, *x) for k, x in enumerate(send)],
            [lambda k=k, x=x: copy(k, x, other) for k, x in enumerate(recv)],
        )

    QKV_STAGES = (
        (((), (0, 1, 4, 8)),),
        (((0,), (2, 5, 9)), ((1,), (3, 6, 10))),
        (((2, 3), (7, 11, 16)),),
        (((4,), (12,)), ((5,), (13,)), ((10,), (14,))),
        (((11,), (15,)), ((6, 7), (17,)), ((8, 9), (18,))),
        (((12, 13, 14, 15), (19,)),),
        (((16, 17, 18, 19), ()),),
    )

    def qkv_stage(k):
        for waits, starts in QKV_STAGES[k]:
            for v in (0, 1):
                send, recv = qkv_copies(v)
                for i in waits:
                    recv[i]().wait_recv()
                for i in starts:
                    send[i]().start()

    def unit_copies(r, v):
        w = weights[r]
        u = 2 * r + v
        c0, c1, ch, (a, ap, am, ao), (b, bp, bm, bo), at, dev, copy = ring(
            w, SPLIT, v, us.at[u], ur.at[u]
        )

        send = [
            lambda: copy(0, at(a, b, c0, c1), dev(ap, b)),
            lambda: copy(1, at(a, b, c0, c1), dev(am, b)),
            lambda: copy(2, at(am, b, c0, ch), dev(ap, b)),
            lambda: copy(3, at(ap, b, ch, c1), dev(am, b)),
            lambda: copy(4, at(slice(None), b, c0, c1), dev(a, bp)),
            lambda: copy(5, at(slice(None), b, c0, c1), dev(a, bm)),
            lambda: copy(6, at(pl.ds(0, 2), bm, c0, c1), dev(a, bp)),
            lambda: copy(7, at(pl.ds(2, 2), bp, c0, c1), dev(a, bm)),
            lambda: copy(8, w.at[:, :, mc, :, pl.ds(c0, c1 - c0)], other),
        ]
        recv = [
            lambda: copy(0, at(am, b, c0, c1), dev(ap, b)),
            lambda: copy(1, at(ap, b, c0, c1), dev(am, b)),
            lambda: copy(2, at(ao, b, c0, ch), dev(ap, b)),
            lambda: copy(3, at(ao, b, ch, c1), dev(am, b)),
            lambda: copy(4, at(slice(None), bm, c0, c1), dev(a, bp)),
            lambda: copy(5, at(slice(None), bp, c0, c1), dev(a, bm)),
            lambda: copy(6, at(pl.ds(0, 2), bo, c0, c1), dev(a, bp)),
            lambda: copy(7, at(pl.ds(2, 2), bo, c0, c1), dev(a, bm)),
            lambda: copy(8, w.at[:, :, 1 - mc, :, pl.ds(c0, c1 - c0)], other),
        ]
        return send, recv

    def step(r, k):
        for i in (0, 1):
            for v in (0, 1):
                send, recv = unit_copies(r, v)
                if k == 1:
                    send[i]().start()
                elif k in (2, 4):
                    recv[2 * k - 4 + i]().wait_recv()
                    send[2 * k - 2 + i]().start()
                elif k in (3, 5):
                    if i == 0:
                        recv[2 * k - 4]().wait_recv()
                        recv[2 * k - 3]().wait_recv()
                        if k == 5:
                            send[8]().start()
                    if k == 3:
                        send[4 + i]().start()
                elif k == 6 and i == 0:
                    recv[8]().wait_recv()

    for c in own_q:
        c.wait()
    qkv_stage(0)

    load(6).wait()
    load(7).wait()

    def wo_copy(k, owner, to):
        part = wo.at[mz, my, mc, :, pl.ds(pl.multiple_of(owner * LW, 128), LW)]
        return rc(part, part, wos.at[k], wor.at[k], {"tensor": to})

    wo_sends = [wo_copy(0, me, right), wo_copy(1, me, left), wo_copy(2, me, opp)]
    wo_recvs = [wo_copy(0, left, right), wo_copy(1, right, left), wo_copy(2, opp, opp)]
    for c in wo_sends:
        c.start()

    load(0).wait()
    load(1).wait()
    emb[...] = jnp.zeros_like(emb)

    def high_low(v):
        high = v.astype(BF)
        return high, (v - high.astype(F32)).astype(BF)

    def embed(n, carry):
        base = pl.multiple_of(n * 512, 512)
        table = jnp.concatenate(high_low(quant[:, pl.ds(base, 512)]), axis=0)
        ids = lax.broadcasted_iota(jnp.int32, (512, PREVTOK), 0) + base
        for j in range(IMGS):
            onehot = jnp.where(tok[j : j + 1, :] == ids, 1.0, 0.0).astype(BF)
            emb[j] += dot(table, onehot)
        return carry

    lax.fori_loop(0, 5, embed, 0)
    qkv_stage(1)
    own_u.wait()
    step(1, 1)
    lax.fori_loop(5, 8, embed, 0)
    qkv_stage(2)
    step(2, 1)

    def modulated(rows_value, scale, shift):
        center = rows_value - jnp.mean(rows_value, axis=-1, keepdims=True)
        variance = jnp.mean(center * center, axis=-1, keepdims=True)
        return (center * lax.rsqrt(variance + FLOOR) * (1.0 + scale) + shift).astype(BF)

    for k in (12, 2, 3, 4, 5):
        load(k).wait()

    ORDER = (2, 1, 3, 0)

    def first_norm(jj, carry):
        j = lax.rem(me + pick(jj, ORDER), NX)
        rows = emb[j, 0:CVAE, :] + emb[j, CVAE : 2 * CVAE, :]
        lifted = lax.dot_general(
            rows, kron[...], (((1,), (0,)), ((), ())),
            precision=lax.Precision.HIGHEST, preferred_element_type=F32,
        )
        can = canv[j] + lifted
        cout[j] = can
        can_hi, can_lo = high_low(can)
        can3 = jnp.concatenate([can_hi, can_lo, can_hi], axis=0)
        for n in range(3):
            cols = slice(n * 512, (n + 1) * 512)
            lift_hi, lift_lo = high_low(lift[:, cols])
            lift3 = jnp.concatenate([lift_hi, lift_hi, lift_lo], axis=0)
            st[:, cols] = loc[:, cols] + lax.dot_general(
                can3, lift3, (((0,), (0,)), ((), ())), preferred_element_type=F32
            )
        scale = fac[2, pl.ds(j, 1), :]
        shift = fac[4, pl.ds(j, 1), :]

        def rows_norm(m, c):
            r = pl.ds(pl.multiple_of(m * 64, 64), 64)
            nb1[j, r, :] = modulated(st[r, :], scale, shift)
            return c

        lax.fori_loop(0, 4, rows_norm, 0)

        @pl.when(jj == 0)
        def _():
            qkv_stage(3)
            for c in wo_recvs:
                c.wait_recv()
            step(0, 1)

        @pl.when(jj == 1)
        def _():
            qkv_stage(4)
            step(0, 2)

        @pl.when(jj == 2)
        def _():
            step(1, 2)

        @pl.when(jj == 3)
        def _():
            qkv_stage(5)
            step(0, 3)
            step(2, 2)

        return carry

    lax.fori_loop(0, 4, first_norm, 0)
    out_canvas = pltpu.make_async_copy(cout, canvas_o, cout_sem.at[0])
    out_canvas.start()

    load(8).wait()
    load(9).wait()

    def to_head(lanes):
        return (
            (lanes >= HDIM).astype(jnp.int32)
            + (lanes >= 2 * HDIM).astype(jnp.int32)
            + (lanes >= 3 * HDIM).astype(jnp.int32)
        )

    block_ones = jnp.where(to_head(lax.broadcasted_iota(jnp.int32, (LW, LW), 0))
        == to_head(lax.broadcasted_iota(jnp.int32, (LW, LW), 1)), 1.0, 0.0).astype(BF)
    lane_row = to_head(lax.broadcasted_iota(jnp.int32, (1, LW), 1))
    sharp = jnp.where(
        lane_row == 0,
        sharp_s[0, 0],
        jnp.where(lane_row == 1, sharp_s[0, 1], jnp.where(lane_row == 2, sharp_s[0, 2], sharp_s[0, 3])),
    )

    def unit(u):
        return u * lax.rsqrt(dot((u * u).astype(BF), block_ones) + 1.0)

    def cache_keys(j, carry):
        knc[j] = unit(kc[j].astype(F32)).astype(BF)
        return carry

    lax.fori_loop(0, 4, cache_keys, 0)
    qkv_stage(6)
    step(1, 3)

    def att_copy(jj, owner, to):
        return rc(att.at[jj], attr.at[owner], ats.at[jj], atr.at[jj], {"tensor": to})

    def attend(jj, carry):
        off = pick(jj, ORDER)
        j = lax.rem(me + off, NX)
        x = nb1[j]
        q = dot(x, wq[:, :, :, :, 0:LW].reshape(D, LW))
        qn[...] = (unit(q) * sharp).astype(BF)
        k = dot(x, wq[:, :, :, :, LW : 2 * LW].reshape(D, LW))
        kn[...] = unit(k).astype(BF)
        vn[...] = dot(x, wq[:, :, :, :, 2 * LW : 3 * LW].reshape(D, LW)).astype(BF)
        for h in range(HEADS_L):
            w0, w1 = WINDOWS[h]
            lanes = lax.broadcasted_iota(jnp.int32, (TOK, w1 - w0), 1) + w0
            mine = (lanes >= h * HDIM) & (lanes < (h + 1) * HDIM)
            qh = jnp.where(mine, qn[:, w0:w1], jnp.zeros((), BF))
            sc = dot_nt(qh, knc[j, :, w0:w1])
            sn = dot_nt(qh, kn[:, w0:w1])
            top = jnp.maximum(
                jnp.max(sc, axis=-1, keepdims=True), jnp.max(sn, axis=-1, keepdims=True)
            )
            pc = jnp.exp(sc - top)
            pn = jnp.exp(sn - top)
            total = jnp.sum(pc, axis=-1, keepdims=True) + jnp.sum(pn, axis=-1, keepdims=True)
            o = dot(pc.astype(BF), vc[j, :, w0:w1]) + dot(pn.astype(BF), vn[:, w0:w1])
            o = (o * (1.0 / total)).astype(BF)
            if h == 0:
                att[jj, :, w0:w1] = o
            else:
                att[jj, :, w0:w1] = jnp.where(mine, o, att[jj, :, w0:w1])

        @pl.when(jj == 0)
        def _():
            step(0, 4)

        @pl.when(jj == 1)
        def _():
            step(2, 3)

        @pl.when(jj == 2)
        def _():
            step(1, 4)

        @pl.when(jj < 3)
        def _():
            att_copy(jj, me, j).start()

        return carry

    att[...] = jnp.zeros_like(att)
    lax.fori_loop(0, 4, attend, 0)
    attr[me] = att[3]
    step(0, 5)
    for jj in range(3):
        att_copy(jj, lax.rem(me + 4 - ORDER[jj], NX), opp).wait_recv()
    step(2, 4)
    step(0, 6)

    def mix(z, carry):
        cols = pl.ds(pl.multiple_of(z * LW, 128), LW)
        mixed = jnp.zeros((TOK, LW), F32)
        for g in range(NX):
            w = wo[z, :, :, :, g * LW : (g + 1) * LW].reshape(LW, LW)
            mixed = mixed + dot_nt(attr[g], w).astype(BF).astype(F32)
        st[:, cols] = st[:, cols] + fac[0, pl.ds(me, 1), cols] * mixed
        return carry

    lax.fori_loop(0, 4, mix, 0)

    scale2 = fac[3, pl.ds(me, 1), :]
    shift2 = fac[5, pl.ds(me, 1), :]

    def second_norm(m, c):
        r = pl.ds(pl.multiple_of(m * 64, 64), 64)
        nb2[me, r, :] = modulated(st[r, :], scale2, shift2)
        return c

    def rows_at(first, count):
        return pl.ds(first, count)

    def gather_copies(nb, ss, rs):
        def c(k, img, first, count, to):
            ref = nb.at[img, rows_at(first, count), :]
            return rc(ref, ref, ss.at[k], rs.at[k], {"tensor": to})

        send, recv = [], []
        for k, first in ((0, 0), (2, HALF)):
            send += [c(k, me, first, HALF, right), c(k + 1, me, first, HALF, left)]
            recv += [c(k, left, first, HALF, right), c(k + 1, right, first, HALF, left)]
        for k, first in ((4, 0), (6, HALF)):
            send += [c(k, left, first, QUART, right), c(k + 1, right, first + QUART, QUART, left)]
            recv += [c(k, opp, first, QUART, right), c(k + 1, opp, first + QUART, QUART, left)]
        return send, recv

    def pass_on(b, send, recv):
        for i in (0, 1):
            recv[2 * b + i].wait_recv()
            send[4 + 2 * b + i].start()

    def blocks(s):
        ia = lax.rem(me + pick(s, (0, 3, 3, 2)), NX)
        ib = lax.rem(me + pick(s, (0, 1, 1, 2)), NX)
        ha = pick(s, (0, 0, 1, 0))
        hb = pick(s, (1, 0, 1, 1))
        ra = pl.ds(pl.multiple_of(ha * HALF, HALF), HALF)
        rb = pl.ds(pl.multiple_of(hb * HALF, HALF), HALF)
        return ia, ra, ib, rb

    send2, recv2 = gather_copies(nb2, g2s, g2r)
    for b in (0, 1):
        lax.fori_loop(2 * b, 2 * b + 2, second_norm, 0)
        send2[2 * b].start()
        send2[2 * b + 1].start()
    step(1, 5)
    step(1, 6)

    def part(k, src, dst, to):
        return rc(src, dst, rss.at[k], rsr.at[k], {"tensor": to})

    def partial_copies(b):
        f = b * HALF
        mine = pbuf.at[1 + b]
        far = pbuf.at[3]
        low, high = rows_at(f, QUART), rows_at(f + QUART, QUART)
        k = 6 * b
        send = [
            part(k, mine.at[rows_at(HALF + QUART, QUART), :], precv.at[0, high, :], right),
            part(k + 1, mine.at[rows_at(0, QUART), :], precv.at[1, low, :], left),
            part(k + 2, far.at[low, :], pacc.at[0, rows_at(b * QUART, QUART), :], right),
            part(k + 3, far.at[high, :], pacc.at[1, rows_at(b * QUART, QUART), :], left),
            part(k + 4, mine.at[rows_at(HALF, QUART), :], precv.at[0, low, :], right),
            part(k + 5, mine.at[rows_at(QUART, QUART), :], precv.at[1, high, :], left),
        ]
        return send

    parts = [partial_copies(b) for b in (0, 1)]

    def feed_forward(s, carry):
        @pl.when(s == 2)
        def _():
            pass_on(1, send2, recv2)
            parts[0][0].start()
            parts[0][1].start()

        @pl.when(s == 3)
        def _():
            for k in range(4, 8):
                recv2[k].wait_recv()

        ia, ra, ib, rb = blocks(s)

        def widen(n, c):
            cols = pl.ds(pl.multiple_of(n * LW, 128), LW)
            x = jnp.concatenate([nb2[ia, ra, :], nb2[ib, rb, :]], axis=0)
            u = dot(x, wu[:, :, :, :, cols].reshape(D, LW))
            act = 0.5 * u * (1.0 + jnp.tanh(0.7978845608028654 * (u + 0.044715 * (u * u * u))))
            hid[:, cols] = act.astype(BF)
            return c

        lax.fori_loop(0, 4, widen, 0)

        @pl.when(s == 0)
        def _():
            pass_on(0, send2, recv2)
            step(2, 5)
            step(2, 6)

        def narrow(z, c):
            cols = pl.ds(pl.multiple_of(z * LW, 128), LW)
            pbuf[s, :, cols] = dot_nt(hid[...], wd[z].reshape(LW, D)).astype(BF)
            return c

        lax.fori_loop(0, 4, narrow, 0)

        @pl.when(s == 2)
        def _():
            parts[1][0].start()
            parts[1][1].start()

        return carry

    lax.fori_loop(0, 4, feed_forward, 0)
    for b in (0, 1):
        parts[b][2].start()
        parts[b][3].start()
    load(10).wait()
    load(11).wait()

    for b in (0, 1):
        came = rows_at(b * QUART, QUART)
        for side, first in ((0, HALF), (1, QUART)):
            parts[b][2 + side].wait_recv()
            rows = rows_at(first, QUART)
            pbuf[1 + b, rows, :] = (
                pbuf[1 + b, rows, :].astype(F32) + pacc[side, came, :].astype(F32)
            ).astype(BF)
            parts[b][4 + side].start()

    gamma2 = fac[1, pl.ds(me, 1), :]
    scale3 = fin[me, 0:1, :]
    shift3 = fin[me, 1:2, :]

    def third_norm(m, c):
        r = pl.ds(pl.multiple_of(m * 64, 64), 64)
        mixed = pbuf[0, r, :].astype(F32) + precv[0, r, :].astype(F32) + precv[1, r, :].astype(F32)
        nb3[me, r, :] = modulated(st[r, :] + gamma2 * mixed, scale3, shift3)
        return c

    send3, recv3 = gather_copies(nb3, g3s, g3r)
    for b in (0, 1):
        for k in (0, 1, 4, 5):
            parts[b][k].wait_recv()
        lax.fori_loop(2 * b, 2 * b + 2, third_norm, 0)
        send3[2 * b].start()
        send3[2 * b + 1].start()

    H = (rows_at(0, HALF), rows_at(HALF, HALF))

    def out_copy(s, k, img, rows):
        return pltpu.make_async_copy(
            lout.at[s, H[k], :], logits_h.at[img, rows, :], out_sem.at[2 * s + k]
        )

    def head(s, carry):
        @pl.when(s == 1)
        def _():
            pass_on(0, send3, recv3)

        @pl.when(s == 2)
        def _():
            pass_on(1, send3, recv3)

        @pl.when(s == 3)
        def _():
            for k in range(4, 8):
                recv3[k].wait_recv()

        ia, ra, ib, rb = blocks(s)

        def tile(n, c):
            cols = pl.ds(pl.multiple_of(n * 256, 256), 256)
            x = jnp.concatenate([nb3[ia, ra, :], nb3[ib, rb, :]], axis=0)
            lout[s, :, cols] = dot(x, voc[:, cols]).astype(BF)
            return c

        lax.fori_loop(0, 4, tile, 0)
        out_copy(s, 0, ia, ra).start()
        out_copy(s, 1, ib, rb).start()
        return carry

    lax.fori_loop(0, 4, head, 0)

    for v in (0, 1):
        send, _ = qkv_copies(v)
        for c in send:
            c().wait_send()
    for r in range(3):
        for v in (0, 1):
            send, _ = unit_copies(r, v)
            for k in range(9):
                send[k]().wait_send()
    for c in wo_sends:
        c.wait_send()
    for jj in range(3):
        att_copy(jj, me, opp).wait_send()
    for k in range(8):
        send2[k].wait_send()
        send3[k].wait_send()
    for b in (0, 1):
        for c in parts[b]:
            c.wait_send()
    out_canvas.wait()

    def out_done(s, carry):
        ia, ra, ib, rb = blocks(s)
        out_copy(s, 0, ia, ra).wait()
        out_copy(s, 1, ib, rb).wait()
        return carry

    lax.fori_loop(0, 4, out_done, 0)


def local(
    sampled_earlier_tokens,
    quantizer_vectors,
    summed_latent_canvas,
    latent_lift_matrix,
    location_tier_offset,
    adaptive_norm_factors,
    logit_sharpness,
    probe_match_content_matrix,
    mixing_projection_matrix,
    widening_projection_matrix,
    narrowing_projection_matrix,
    cached_lower_grid_lookups,
    cached_lower_grid_payloads,
    final_norm_factors,
    vocabulary_logit_matrix,
):
    operands = (
        sampled_earlier_tokens,
        quantizer_vectors.T,
        jnp.swapaxes(summed_latent_canvas, 1, 2),
        latent_lift_matrix,
        location_tier_offset,
        jnp.swapaxes(adaptive_norm_factors[0], 0, 1),
        logit_sharpness,
        jnp.swapaxes(probe_match_content_matrix[0], 0, 1),
        mixing_projection_matrix[0].T,
        widening_projection_matrix[0],
        narrowing_projection_matrix[0].T,
        cached_lower_grid_lookups[0],
        cached_lower_grid_payloads[0],
        final_norm_factors,
        vocabulary_logit_matrix,
        jnp.asarray(upsample_matrix()),
    )
    anyspace = pl.BlockSpec(memory_space=pl.ANY)
    specs = [anyspace] * len(operands)
    specs[6] = pl.BlockSpec(memory_space=pltpu.SMEM)
    vm = pltpu.VMEM
    dma = pltpu.SemaphoreType.DMA
    scratch = [
        vm((IMGS, PREVTOK), jnp.int32),
        vm((CVAE, VOCAB), F32),
        vm((IMGS, CVAE, TOK), F32),
        vm((CVAE, D), F32),
        vm((TOK, D), F32),
        vm((6, IMGS, D), F32),
        vm((IMGS, CACHE, LW), BF),
        vm((IMGS, CACHE, LW), BF),
        vm((IMGS, 2, D), F32),
        vm((D, VL), BF),
        vm((PREVTOK, TOK), F32),
        vm((4, 4, 2, SH, 3 * LW), BF),
        vm((4, 4, 2, SH, D), BF),
        vm((4, 4, 2, SH, D), BF),
        vm((4, 4, 2, SH, D), BF),
        vm((IMGS, 2 * CVAE, PREVTOK), F32),
        vm((IMGS, CVAE, TOK), F32),
        vm((TOK, D), F32),
        vm((IMGS, TOK, D), BF),
        vm((IMGS, TOK, D), BF),
        vm((IMGS, TOK, D), BF),
        vm((TOK, LW), BF),
        vm((TOK, LW), BF),
        vm((TOK, LW), BF),
        vm((IMGS, CACHE, LW), BF),
        vm((NX, TOK, LW), BF),
        vm((NX, TOK, LW), BF),
        vm((TOK, D), BF),
        vm((NX, TOK, D), BF),
        vm((2, TOK, D), BF),
        vm((2, HALF, D), BF),
        vm((NX, TOK, VL), BF),
        dma((13,)), dma((4,)), dma((8,)), dma((1,)),
        dma((2, 20)), dma((2, 20)), dma((6, 9)), dma((6, 9)), dma((3,)), dma((3,)), dma((3,)), dma((3,)),
        dma((8,)), dma((8,)), dma((12,)), dma((12,)), dma((8,)), dma((8,)),
    ]
    logits, canvas = pl.pallas_call(
        body,
        out_shape=(
            jax.ShapeDtypeStruct((IMGS, TOK, VL), BF),
            jax.ShapeDtypeStruct((IMGS, CVAE, TOK), F32),
        ),
        in_specs=specs,
        out_specs=(anyspace, anyspace),
        scratch_shapes=scratch,
        compiler_params=pltpu.CompilerParams(
            collective_id=0, has_side_effects=True, vmem_limit_bytes=67_000_000
        ),
    )(*operands)
    return logits, jnp.swapaxes(canvas, 1, 2)


def solution(mesh):
    placed = (
        P("dp", None),
        P(),
        P("dp", None, None),
        P(),
        P(),
        P(None, "dp", None, None),
        P(None, "tensor"),
        P(None, "dp", None, "tensor"),
        P(None, "tensor", "dp"),
        P(None, "dp", "tensor"),
        P(None, "tensor", "dp"),
        P(None, "dp", None, "tensor"),
        P(None, "dp", None, "tensor"),
        P("dp", None, None),
        P(None, "tensor"),
    )
    return jax.shard_map(
        local,
        mesh=mesh,
        in_specs=placed,
        out_specs=(P("dp", None, "tensor"), P("dp", None, None)),
        check_vma=False,
    )
```

```python
import numpy as np
import jax
import jax.numpy as jnp
from jax import lax
from jax.experimental import pallas as pl
from jax.experimental.pallas import tpu as pltpu
from jax.sharding import PartitionSpec as P

MESH = pl.DeviceIdType.MESH
BF = jnp.bfloat16
F32 = jnp.float32

D = 1536
HEADS_L = 4
HDIM = 96
LW = HEADS_L * HDIM
VOCAB = 4096
VL = 1024
CVAE = 32
SIDE = 16
PREV = 13
PREVTOK = 169
CACHE = 424
TOK = 256
HALF = 128
QUART = 64
IMGS = 4
SH = 48
NX = 4
FLOOR = 0.1

WINDOWS = ((0, 128), (0, 256), (128, 384), (256, 384))

QKV_SPLIT = ((0, 640, 384), (640, 1152, 896))
SPLIT = ((0, 768, 384), (768, 1536, 1152))


def upsample_matrix():
    a = np.arange(SIDE)
    num = np.maximum((2 * a + 1) * PREV - SIDE, 0)
    low = num // (2 * SIDE)
    frac = (num % (2 * SIDE)) / (2.0 * SIDE)
    up = np.zeros((SIDE, PREV))
    up[a, low] += 1.0 - frac
    up[a, np.minimum(low + 1, PREV - 1)] += frac
    return np.kron(up, up).T.astype(np.float32)


def dot(a, b):
    return jnp.dot(a, b, preferred_element_type=F32)


def dot_nt(a, b):
    return lax.dot_general(a, b, (((1,), (1,)), ((), ())), preferred_element_type=F32)


def pick(index, values):
    out = values[-1]
    for k in range(len(values) - 1):
        out = jnp.where(index == k, values[k], out)
    return out


def body(
    tok_h, quant_h, canvas_h, lift_h, loc_h, fac_h, sharp_s, qkv_h, wo_h, up_h, wd_h,
    kc_h, vc_h, fin_h, voc_h, kron_h,
    logits_o, canvas_o,
    tok, quant, canv, lift, loc, fac, kc, vc, fin, voc, kron,
    wq, wo, wu, wd,
    emb, st, nb1, nb2, nb3, qn, kn, vn, knc, att, attr, hid, pbuf, precv, pacc,
    load_sem, own_sem,
    qs, qr, us, ur, wos, wor, ats, atr, g2s, g2r, rss, rsr, g3s, g3r,
):
    me = lax.axis_index("tensor")
    dp = lax.axis_index("dp")
    mz = dp // 8
    my = lax.rem(dp // 2, 4)
    mc = lax.rem(dp, 2)
    right = lax.rem(me + 1, NX)
    left = lax.rem(me + 3, NX)
    opp = lax.rem(me + 2, NX)
    yp, ym, yo = lax.rem(my + 1, 4), lax.rem(my + 3, 4), lax.rem(my + 2, 4)
    zp, zm, zo = lax.rem(mz + 1, 4), lax.rem(mz + 3, 4), lax.rem(mz + 2, 4)

    def dpi(z, y, c):
        return {"dp": (z * 4 + y) * 2 + c}

    def rc(src, dst, s, r, dev):
        return pltpu.make_async_remote_copy(
            src_ref=src, dst_ref=dst, send_sem=s, recv_sem=r, device_id=dev, device_id_type=MESH
        )

    mycols = pl.ds(pl.multiple_of(me * LW, 128), LW)
    loads = [
        (tok_h, tok), (quant_h, quant), (canvas_h, canv), (lift_h, lift), (loc_h, loc),
        (fac_h, fac), (wo_h, wo.at[mz, my, mc, :, mycols]), (wd_h, wd.at[mz, my, mc]),
        (kc_h, kc), (vc_h, vc), (fin_h, fin), (voc_h, voc), (kron_h, kron),
    ]

    def load(k):
        return pltpu.make_async_copy(loads[k][0], loads[k][1], load_sem.at[k])

    own_q = [
        pltpu.make_async_copy(
            qkv_h.at[k], wq.at[mz, my, mc, :, pl.ds(k * LW, LW)], own_sem.at[1 + k]
        )
        for k in range(3)
    ]
    own_u = pltpu.make_async_copy(up_h, wu.at[mz, my, mc], own_sem.at[0])
    for c in own_q:
        c.start()
    for k in (6, 7, 0, 1, 12, 2, 3, 4, 5):
        load(k).start()
    own_u.start()
    for k in (8, 9, 10, 11):
        load(k).start()

    barrier = pltpu.get_barrier_semaphore()
    peers = [{"tensor": right}, {"tensor": left}, {"tensor": opp}]
    peers += [dpi(mz, yp, mc), dpi(mz, ym, mc), dpi(mz, yo, mc), dpi(zp, my, mc), dpi(zm, my, mc)]
    peers += [dpi(zo, my, mc), dpi(mz, my, 1 - mc)]
    for dev in peers:
        pl.semaphore_signal(barrier, inc=1, device_id=dev, device_id_type=MESH)
    pl.semaphore_wait(barrier, len(peers))

    weights = (wo, wu, wd)

    def ring(w, split, v, sends, recvs):
        c0, c1, ch = split[v]
        a, ap, am, ao = (my, yp, ym, yo) if v == 0 else (mz, zp, zm, zo)
        b, bp, bm, bo = (mz, zp, zm, zo) if v == 0 else (my, yp, ym, yo)

        def at(ai, bi, lo, hi, core=mc):
            cols = pl.ds(lo, hi - lo)
            return w.at[bi, ai, core, :, cols] if v == 0 else w.at[ai, bi, core, :, cols]

        def dev(ai, bi):
            return dpi(bi, ai, mc) if v == 0 else dpi(ai, bi, mc)

        def copy(k, src, to):
            return rc(src, src, sends.at[k], recvs.at[k], to)

        return c0, c1, ch, (a, ap, am, ao), (b, bp, bm, bo), at, dev, copy

    other = dpi(mz, my, 1 - mc)

    def qkv_copies(v):
        c0, c1, ch, (a, ap, am, ao), (b, bp, bm, bo), at, dev, copy = ring(
            wq, QKV_SPLIT, v, qs.at[v], qr.at[v]
        )
        every = slice(None)
        row = (a, am, ap, ao)
        send = [
            (at(a, b, c0, c1), dev(ap, b)),
            (at(a, b, c0, c1), dev(am, b)),
            (at(a, b, c0, ch), dev(ao, b)),
            (at(a, b, ch, c1), dev(ao, b)),
        ]
        recv = [at(am, b, c0, c1), at(ap, b, c0, c1), at(ao, b, c0, ch), at(ao, b, ch, c1)]
        send += [(at(ai, b, c0, c1), dev(a, bp)) for ai in row]
        recv += [at(ai, bm, c0, c1) for ai in row]
        send += [(at(ai, b, c0, c1), dev(a, bm)) for ai in row]
        recv += [at(ai, bp, c0, c1) for ai in row]
        send += [(at(ai, bm, c0, c1), dev(a, bp)) for ai in row[:2]]
        send += [(at(ai, bp, c0, c1), dev(a, bm)) for ai in row[2:]]
        recv += [at(ai, bo, c0, c1) for ai in row]
        send += [(at(every, bi, c0, c1), other) for bi in (b, bm, bp, bo)]
        recv += [at(every, bi, c0, c1, 1 - mc) for bi in (b, bm, bp, bo)]
        return (
            [lambda k=k, x=x: copy(k, *x) for k, x in enumerate(send)],
            [lambda k=k, x=x: copy(k, x, other) for k, x in enumerate(recv)],
        )

    QKV_STAGES = (
        (((), (0, 1, 2, 3, 4, 8)),),
        (((0,), (5, 9)), ((1,), (6, 10))),
        (((2, 3), (7, 11, 16)),),
        (((4,), (12,)), ((5,), (13,)), ((10,), (14,))),
        (((11,), (15,)), ((6, 7), (17,)), ((8, 9), (18,))),
        (((12, 13, 14, 15), (19,)),),
        (((16, 17, 18, 19), ()),),
    )

    def qkv_stage(k):
        for waits, starts in QKV_STAGES[k]:
            for v in (0, 1):
                send, recv = qkv_copies(v)
                for i in waits:
                    recv[i]().wait_recv()
                for i in starts:
                    send[i]().start()

    def unit_copies(r, v):
        w = weights[r]
        u = 2 * r + v
        c0, c1, ch, (a, ap, am, ao), (b, bp, bm, bo), at, dev, copy = ring(
            w, SPLIT, v, us.at[u], ur.at[u]
        )

        send = [
            lambda: copy(0, at(a, b, c0, c1), dev(ap, b)),
            lambda: copy(1, at(a, b, c0, c1), dev(am, b)),
            lambda: copy(2, at(am, b, c0, ch), dev(ap, b)),
            lambda: copy(3, at(ap, b, ch, c1), dev(am, b)),
            lambda: copy(4, at(slice(None), b, c0, c1), dev(a, bp)),
            lambda: copy(5, at(slice(None), b, c0, c1), dev(a, bm)),
            lambda: copy(6, at(pl.ds(0, 2), bm, c0, c1), dev(a, bp)),
            lambda: copy(7, at(pl.ds(2, 2), bp, c0, c1), dev(a, bm)),
            lambda: copy(8, w.at[:, :, mc, :, pl.ds(c0, c1 - c0)], other),
        ]
        recv = [
            lambda: copy(0, at(am, b, c0, c1), dev(ap, b)),
            lambda: copy(1, at(ap, b, c0, c1), dev(am, b)),
            lambda: copy(2, at(ao, b, c0, ch), dev(ap, b)),
            lambda: copy(3, at(ao, b, ch, c1), dev(am, b)),
            lambda: copy(4, at(slice(None), bm, c0, c1), dev(a, bp)),
            lambda: copy(5, at(slice(None), bp, c0, c1), dev(a, bm)),
            lambda: copy(6, at(pl.ds(0, 2), bo, c0, c1), dev(a, bp)),
            lambda: copy(7, at(pl.ds(2, 2), bo, c0, c1), dev(a, bm)),
            lambda: copy(8, w.at[:, :, 1 - mc, :, pl.ds(c0, c1 - c0)], other),
        ]
        return send, recv

    def step(r, k):
        for i in (0, 1):
            for v in (0, 1):
                send, recv = unit_copies(r, v)
                if k == 1:
                    send[i]().start()
                elif k in (2, 4):
                    recv[2 * k - 4 + i]().wait_recv()
                    send[2 * k - 2 + i]().start()
                elif k in (3, 5):
                    if i == 0:
                        recv[2 * k - 4]().wait_recv()
                        recv[2 * k - 3]().wait_recv()
                        if k == 5:
                            send[8]().start()
                    if k == 3:
                        send[4 + i]().start()
                elif k == 6 and i == 0:
                    recv[8]().wait_recv()

    for c in own_q:
        c.wait()
    qkv_stage(0)

    load(6).wait()
    load(7).wait()
    own_u.wait()
    step(1, 1)

    def wo_copy(k, owner, to):
        part = wo.at[mz, my, mc, :, pl.ds(pl.multiple_of(owner * LW, 128), LW)]
        return rc(part, part, wos.at[k], wor.at[k], {"tensor": to})

    wo_sends = [wo_copy(0, me, right), wo_copy(1, me, left), wo_copy(2, me, opp)]
    wo_recvs = [wo_copy(0, left, right), wo_copy(1, right, left), wo_copy(2, opp, opp)]
    for c in wo_sends:
        c.start()

    load(0).wait()
    load(1).wait()
    emb[...] = jnp.zeros_like(emb)

    def high_low(v):
        high = v.astype(BF)
        return high, (v - high.astype(F32)).astype(BF)

    def embed(n, carry):
        base = pl.multiple_of(n * 512, 512)
        table = jnp.concatenate(high_low(quant[:, pl.ds(base, 512)]), axis=0)
        ids = lax.broadcasted_iota(jnp.int32, (512, PREVTOK), 0) + base
        for j in range(IMGS):
            onehot = jnp.where(tok[j : j + 1, :] == ids, 1.0, 0.0).astype(BF)
            emb[j] += dot(table, onehot)
        return carry

    lax.fori_loop(0, 5, embed, 0)
    qkv_stage(1)
    step(2, 1)
    lax.fori_loop(5, 8, embed, 0)
    qkv_stage(2)
    for c in wo_recvs:
        c.wait_recv()
    step(0, 1)

    def modulated(rows_value, scale, shift):
        center = rows_value - jnp.mean(rows_value, axis=-1, keepdims=True)
        variance = jnp.mean(center * center, axis=-1, keepdims=True)
        return (center * lax.rsqrt(variance + FLOOR) * (1.0 + scale) + shift).astype(BF)

    for k in (12, 2, 3, 4, 5):
        load(k).wait()

    ORDER = (2, 1, 3, 0)

    def first_norm(jj, carry):
        j = lax.rem(me + pick(jj, ORDER), NX)
        rows = emb[j, 0:CVAE, :] + emb[j, CVAE : 2 * CVAE, :]
        lifted = lax.dot_general(
            rows, kron[...], (((1,), (0,)), ((), ())),
            precision=lax.Precision.HIGHEST, preferred_element_type=F32,
        )
        can = canv[j] + lifted
        canvas_o[j] = can
        can_hi, can_lo = high_low(can)
        can3 = jnp.concatenate([can_hi, can_lo, can_hi], axis=0)
        for n in range(3):
            cols = slice(n * 512, (n + 1) * 512)
            lift_hi, lift_lo = high_low(lift[:, cols])
            lift3 = jnp.concatenate([lift_hi, lift_hi, lift_lo], axis=0)
            st[:, cols] = loc[:, cols] + lax.dot_general(
                can3, lift3, (((0,), (0,)), ((), ())), preferred_element_type=F32
            )
        scale = fac[2, pl.ds(j, 1), :]
        shift = fac[4, pl.ds(j, 1), :]

        def rows_norm(m, c):
            r = pl.ds(pl.multiple_of(m * 64, 64), 64)
            nb1[j, r, :] = modulated(st[r, :], scale, shift)
            return c

        lax.fori_loop(0, 4, rows_norm, 0)

        @pl.when(jj == 0)
        def _():
            qkv_stage(3)
            step(0, 2)

        @pl.when(jj == 1)
        def _():
            qkv_stage(4)
            step(1, 2)
            step(0, 3)

        @pl.when(jj == 2)
        def _():
            step(2, 2)

        @pl.when(jj == 3)
        def _():
            qkv_stage(5)

        return carry

    lax.fori_loop(0, 4, first_norm, 0)

    load(8).wait()
    load(9).wait()

    def to_head(lanes):
        return (
            (lanes >= HDIM).astype(jnp.int32)
            + (lanes >= 2 * HDIM).astype(jnp.int32)
            + (lanes >= 3 * HDIM).astype(jnp.int32)
        )

    block_ones = jnp.where(to_head(lax.broadcasted_iota(jnp.int32, (LW, LW), 0))
        == to_head(lax.broadcasted_iota(jnp.int32, (LW, LW), 1)), 1.0, 0.0).astype(BF)
    lane_row = to_head(lax.broadcasted_iota(jnp.int32, (1, LW), 1))
    sharp = jnp.where(
        lane_row == 0,
        sharp_s[0, 0],
        jnp.where(lane_row == 1, sharp_s[0, 1], jnp.where(lane_row == 2, sharp_s[0, 2], sharp_s[0, 3])),
    )

    def unit(u):
        return u * lax.rsqrt(dot((u * u).astype(BF), block_ones) + 1.0)

    def cache_keys(j, carry):
        knc[j] = unit(kc[j].astype(F32)).astype(BF)
        return carry

    lax.fori_loop(0, 4, cache_keys, 0)
    qkv_stage(6)

    def att_copy(jj, owner, to):
        return rc(att.at[jj], attr.at[owner], ats.at[jj], atr.at[jj], {"tensor": to})

    def attend(jj, carry):
        off = pick(jj, ORDER)
        j = lax.rem(me + off, NX)
        x = nb1[j]
        q = dot(x, wq[:, :, :, :, 0:LW].reshape(D, LW))
        qn[...] = (unit(q) * sharp).astype(BF)
        k = dot(x, wq[:, :, :, :, LW : 2 * LW].reshape(D, LW))
        kn[...] = unit(k).astype(BF)
        vn[...] = dot(x, wq[:, :, :, :, 2 * LW : 3 * LW].reshape(D, LW)).astype(BF)
        @pl.when(jj == 0)
        def _():
            step(0, 4)
            step(1, 3)

        @pl.when(jj == 1)
        def _():
            step(2, 3)

        @pl.when(jj == 2)
        def _():
            step(0, 5)

        outs = []
        for h in range(HEADS_L):
            w0, w1 = WINDOWS[h]
            lanes = lax.broadcasted_iota(jnp.int32, (TOK, w1 - w0), 1) + w0
            mine = (lanes >= h * HDIM) & (lanes < (h + 1) * HDIM)
            qh = jnp.where(mine, qn[:, w0:w1], jnp.zeros((), BF))
            sc = dot_nt(qh, knc[j, :, w0:w1])
            sn = dot_nt(qh, kn[:, w0:w1])
            top = jnp.maximum(
                jnp.max(sc, axis=-1, keepdims=True), jnp.max(sn, axis=-1, keepdims=True)
            )
            pc = jnp.exp(sc - top)
            pn = jnp.exp(sn - top)
            total = jnp.sum(pc, axis=-1, keepdims=True) + jnp.sum(pn, axis=-1, keepdims=True)
            o = dot(pc.astype(BF), vc[j, :, w0:w1]) + dot(pn.astype(BF), vn[:, w0:w1])
            outs.append(o * (1.0 / total))
        lane = lax.broadcasted_iota(jnp.int32, (TOK, 128), 1)
        for c in range(3):
            w0 = WINDOWS[c + 1][0]
            first = outs[c][:, c * 128 - WINDOWS[c][0] : c * 128 - WINDOWS[c][0] + 128]
            second = outs[c + 1][:, c * 128 - w0 : c * 128 - w0 + 128]
            edge = (c + 1) * HDIM - c * 128
            att[jj, :, c * 128 : (c + 1) * 128] = jnp.where(lane < edge, first, second).astype(BF)

        @pl.when(jj < 3)
        def _():
            att_copy(jj, me, j).start()

        return carry

    lax.fori_loop(0, 4, attend, 0)
    attr[me] = att[3]
    for jj in range(3):
        att_copy(jj, lax.rem(me + 4 - ORDER[jj], NX), opp).wait_recv()
    step(0, 6)
    step(1, 4)

    def mix(z, carry):
        cols = pl.ds(pl.multiple_of(z * LW, 128), LW)
        mixed = jnp.zeros((TOK, LW), F32)
        for g in range(NX):
            w = wo[z, :, :, :, g * LW : (g + 1) * LW].reshape(LW, LW)
            mixed = mixed + dot_nt(attr[g], w).astype(BF).astype(F32)
        st[:, cols] = st[:, cols] + fac[0, pl.ds(me, 1), cols] * mixed
        return carry

    lax.fori_loop(0, 4, mix, 0)

    scale2 = fac[3, pl.ds(me, 1), :]
    shift2 = fac[5, pl.ds(me, 1), :]

    def second_norm(m, c):
        r = pl.ds(pl.multiple_of(m * 64, 64), 64)
        nb2[me, r, :] = modulated(st[r, :], scale2, shift2)
        return c

    def rows_at(first, count):
        return pl.ds(first, count)

    def gather_copies(nb, ss, rs):
        def c(k, img, first, count, to):
            ref = nb.at[img, rows_at(first, count), :]
            return rc(ref, ref, ss.at[k], rs.at[k], {"tensor": to})

        send, recv = [], []
        for k, first in ((0, 0), (2, HALF)):
            send += [c(k, me, first, HALF, right), c(k + 1, me, first, HALF, left)]
            recv += [c(k, left, first, HALF, right), c(k + 1, right, first, HALF, left)]
        for k, first in ((4, 0), (6, HALF)):
            send += [c(k, left, first, QUART, right), c(k + 1, right, first + QUART, QUART, left)]
            recv += [c(k, opp, first, QUART, right), c(k + 1, opp, first + QUART, QUART, left)]
        return send, recv

    def pass_on(b, send, recv):
        for i in (0, 1):
            recv[2 * b + i].wait_recv()
            send[4 + 2 * b + i].start()

    def blocks(s):
        ia = lax.rem(me + pick(s, (0, 3, 3, 2)), NX)
        ib = lax.rem(me + pick(s, (0, 1, 1, 2)), NX)
        ha = pick(s, (0, 0, 1, 0))
        hb = pick(s, (1, 0, 1, 1))
        ra = pl.ds(pl.multiple_of(ha * HALF, HALF), HALF)
        rb = pl.ds(pl.multiple_of(hb * HALF, HALF), HALF)
        return ia, ra, ib, rb

    send2, recv2 = gather_copies(nb2, g2s, g2r)
    for b in (0, 1):
        lax.fori_loop(2 * b, 2 * b + 2, second_norm, 0)
        send2[2 * b].start()
        send2[2 * b + 1].start()
    step(2, 4)
    step(1, 5)

    def part(k, src, dst, to):
        return rc(src, dst, rss.at[k], rsr.at[k], {"tensor": to})

    def partial_copies(b):
        f = b * HALF
        mine = pbuf.at[1 + b]
        far = pbuf.at[3]
        low, high = rows_at(f, QUART), rows_at(f + QUART, QUART)
        k = 6 * b
        send = [
            part(k, mine.at[rows_at(HALF + QUART, QUART), :], precv.at[0, high, :], right),
            part(k + 1, mine.at[rows_at(0, QUART), :], precv.at[1, low, :], left),
            part(k + 2, far.at[low, :], pacc.at[0, rows_at(b * QUART, QUART), :], right),
            part(k + 3, far.at[high, :], pacc.at[1, rows_at(b * QUART, QUART), :], left),
            part(k + 4, mine.at[rows_at(HALF, QUART), :], precv.at[0, low, :], right),
            part(k + 5, mine.at[rows_at(QUART, QUART), :], precv.at[1, high, :], left),
        ]
        return send

    parts = [partial_copies(b) for b in (0, 1)]

    def widen(s):
        ia, ra, ib, rb = blocks(s)

        def tile(n, c):
            cols = pl.ds(pl.multiple_of(n * LW, 128), LW)
            x = jnp.concatenate([nb2[ia, ra, :], nb2[ib, rb, :]], axis=0)
            u = dot(x, wu[:, :, :, :, cols].reshape(D, LW))
            act = 0.5 * u * (1.0 + jnp.tanh(0.7978845608028654 * (u + 0.044715 * (u * u * u))))
            hid[s, :, cols] = act.astype(BF)
            return c

        lax.fori_loop(0, 4, tile, 0)

    def narrow(s):
        def tile(z, c):
            cols = pl.ds(pl.multiple_of(z * LW, 128), LW)
            pbuf[s, :, cols] = dot_nt(hid[s], wd[z].reshape(LW, D)).astype(BF)
            return c

        lax.fori_loop(0, 4, tile, 0)

    pass_on(0, send2, recv2)
    step(1, 6)

    def widen_ready(t, carry):
        s = pick(t, (1, 0, 2, 3))

        @pl.when(t == 1)
        def _():
            step(2, 5)

        @pl.when(t == 2)
        def _():
            pass_on(1, send2, recv2)

        @pl.when(t == 3)
        def _():
            step(2, 6)

            def near(s, c):
                narrow(s)
                return c

            lax.fori_loop(1, 3, near, 0)
            for b in (0, 1):
                parts[b][0].start()
                parts[b][1].start()
            for k in range(4, 8):
                recv2[k].wait_recv()

        widen(s)
        return carry

    lax.fori_loop(0, 4, widen_ready, 0)

    def narrow_last(t, carry):
        @pl.when(t == 1)
        def _():
            for b in (0, 1):
                parts[b][2].start()
                parts[b][3].start()

        narrow(pick(t, (3, 0)))
        return carry

    lax.fori_loop(0, 2, narrow_last, 0)
    load(10).wait()
    load(11).wait()

    for b in (0, 1):
        came = rows_at(b * QUART, QUART)
        for side, first in ((0, HALF), (1, QUART)):
            parts[b][2 + side].wait_recv()
            rows = rows_at(first, QUART)
            pbuf[1 + b, rows, :] = (
                pbuf[1 + b, rows, :].astype(F32) + pacc[side, came, :].astype(F32)
            ).astype(BF)
            parts[b][4 + side].start()

    gamma2 = fac[1, pl.ds(me, 1), :]
    scale3 = fin[me, 0:1, :]
    shift3 = fin[me, 1:2, :]

    def third_norm(m, c):
        r = pl.ds(pl.multiple_of(m * 64, 64), 64)
        mixed = pbuf[0, r, :].astype(F32) + precv[0, r, :].astype(F32) + precv[1, r, :].astype(F32)
        nb3[me, r, :] = modulated(st[r, :] + gamma2 * mixed, scale3, shift3)
        return c

    send3, recv3 = gather_copies(nb3, g3s, g3r)
    for b in (0, 1):
        for k in (0, 1, 4, 5):
            parts[b][k].wait_recv()
        lax.fori_loop(2 * b, 2 * b + 2, third_norm, 0)
        send3[2 * b].start()
        send3[2 * b + 1].start()

    def head(s, carry):
        @pl.when(s == 1)
        def _():
            pass_on(0, send3, recv3)

        @pl.when(s == 2)
        def _():
            pass_on(1, send3, recv3)

        @pl.when(s == 3)
        def _():
            for k in range(4, 8):
                recv3[k].wait_recv()

        ia, ra, ib, rb = blocks(s)

        def tile(n, c):
            cols = pl.ds(pl.multiple_of(n * 256, 256), 256)
            x = jnp.concatenate([nb3[ia, ra, :], nb3[ib, rb, :]], axis=0)
            y = dot(x, voc[:, cols]).astype(BF)
            logits_o[ia, ra, cols] = y[:HALF]
            logits_o[ib, rb, cols] = y[HALF:]
            return c

        lax.fori_loop(0, 4, tile, 0)
        return carry

    lax.fori_loop(0, 4, head, 0)

    for v in (0, 1):
        send, _ = qkv_copies(v)
        for c in send:
            c().wait_send()
    for r in range(3):
        for v in (0, 1):
            send, _ = unit_copies(r, v)
            for k in range(9):
                send[k]().wait_send()
    for c in wo_sends:
        c.wait_send()
    for jj in range(3):
        att_copy(jj, me, opp).wait_send()
    for k in range(8):
        send2[k].wait_send()
        send3[k].wait_send()
    for b in (0, 1):
        for c in parts[b]:
            c.wait_send()


def local(
    sampled_earlier_tokens,
    quantizer_vectors,
    summed_latent_canvas,
    latent_lift_matrix,
    location_tier_offset,
    adaptive_norm_factors,
    logit_sharpness,
    probe_match_content_matrix,
    mixing_projection_matrix,
    widening_projection_matrix,
    narrowing_projection_matrix,
    cached_lower_grid_lookups,
    cached_lower_grid_payloads,
    final_norm_factors,
    vocabulary_logit_matrix,
):
    operands = (
        sampled_earlier_tokens,
        quantizer_vectors.T,
        jnp.swapaxes(summed_latent_canvas, 1, 2),
        latent_lift_matrix,
        location_tier_offset,
        jnp.swapaxes(adaptive_norm_factors[0], 0, 1),
        logit_sharpness,
        jnp.swapaxes(probe_match_content_matrix[0], 0, 1),
        mixing_projection_matrix[0].T,
        widening_projection_matrix[0],
        narrowing_projection_matrix[0].T,
        cached_lower_grid_lookups[0],
        cached_lower_grid_payloads[0],
        final_norm_factors,
        vocabulary_logit_matrix,
        jnp.asarray(upsample_matrix()),
    )
    anyspace = pl.BlockSpec(memory_space=pl.ANY)
    specs = [anyspace] * len(operands)
    specs[6] = pl.BlockSpec(memory_space=pltpu.SMEM)
    vm = pltpu.VMEM
    dma = pltpu.SemaphoreType.DMA
    scratch = [
        vm((IMGS, PREVTOK), jnp.int32),
        vm((CVAE, VOCAB), F32),
        vm((IMGS, CVAE, TOK), F32),
        vm((CVAE, D), F32),
        vm((TOK, D), F32),
        vm((6, IMGS, D), F32),
        vm((IMGS, CACHE, LW), BF),
        vm((IMGS, CACHE, LW), BF),
        vm((IMGS, 2, D), F32),
        vm((D, VL), BF),
        vm((PREVTOK, TOK), F32),
        vm((4, 4, 2, SH, 3 * LW), BF),
        vm((4, 4, 2, SH, D), BF),
        vm((4, 4, 2, SH, D), BF),
        vm((4, 4, 2, SH, D), BF),
        vm((IMGS, 2 * CVAE, PREVTOK), F32),
        vm((TOK, D), F32),
        vm((IMGS, TOK, D), BF),
        vm((IMGS, TOK, D), BF),
        vm((IMGS, TOK, D), BF),
        vm((TOK, LW), BF),
        vm((TOK, LW), BF),
        vm((TOK, LW), BF),
        vm((IMGS, CACHE, LW), BF),
        vm((NX, TOK, LW), BF),
        vm((NX, TOK, LW), BF),
        vm((NX, TOK, D), BF),
        vm((NX, TOK, D), BF),
        vm((2, TOK, D), BF),
        vm((2, HALF, D), BF),
        dma((13,)), dma((4,)),
        dma((2, 20)), dma((2, 20)), dma((6, 9)), dma((6, 9)), dma((3,)), dma((3,)), dma((3,)), dma((3,)),
        dma((8,)), dma((8,)), dma((12,)), dma((12,)), dma((8,)), dma((8,)),
    ]
    logits, canvas = pl.pallas_call(
        body,
        out_shape=(
            pltpu.VMEM((IMGS, TOK, VL), BF),
            pltpu.VMEM((IMGS, CVAE, TOK), F32),
        ),
        in_specs=specs,
        out_specs=(pl.BlockSpec(memory_space=pltpu.VMEM), pl.BlockSpec(memory_space=pltpu.VMEM)),
        scratch_shapes=scratch,
        compiler_params=pltpu.CompilerParams(
            collective_id=0, has_side_effects=True, vmem_limit_bytes=60_000_000
        ),
    )(*operands)
    return logits, jnp.swapaxes(canvas, 1, 2)


def solution(mesh):
    placed = (
        P("dp", None),
        P(),
        P("dp", None, None),
        P(),
        P(),
        P(None, "dp", None, None),
        P(None, "tensor"),
        P(None, "dp", None, "tensor"),
        P(None, "tensor", "dp"),
        P(None, "dp", "tensor"),
        P(None, "tensor", "dp"),
        P(None, "dp", None, "tensor"),
        P(None, "dp", None, "tensor"),
        P("dp", None, None),
        P(None, "tensor"),
    )
    return jax.shard_map(
        local,
        mesh=mesh,
        in_specs=placed,
        out_specs=(P("dp", None, "tensor"), P("dp", None, None)),
        check_vma=False,
    )
```

```python
import numpy as np
import jax
import jax.numpy as jnp
from jax import lax
from jax.experimental import pallas as pl
from jax.experimental.pallas import tpu as pltpu
from jax.sharding import PartitionSpec as P

MESH = pl.DeviceIdType.MESH
BF = jnp.bfloat16
F32 = jnp.float32

D = 1536
HEADS_L = 4
HDIM = 96
LW = HEADS_L * HDIM
VOCAB = 4096
VL = 1024
CVAE = 32
SIDE = 16
PREV = 13
PREVTOK = 169
CACHE = 424
TOK = 256
HALF = 128
QUART = 64
IMGS = 4
SH = 48
NX = 4
FLOOR = 0.1

WINDOWS = ((0, 128), (0, 256), (128, 384), (256, 384))

QKV_SPLIT = ((0, 640, 384), (640, 1152, 896))
SPLIT = ((0, 768, 384), (768, 1536, 1152))


def upsample_matrix():
    a = np.arange(SIDE)
    num = np.maximum((2 * a + 1) * PREV - SIDE, 0)
    low = num // (2 * SIDE)
    frac = (num % (2 * SIDE)) / (2.0 * SIDE)
    up = np.zeros((SIDE, PREV))
    up[a, low] += 1.0 - frac
    up[a, np.minimum(low + 1, PREV - 1)] += frac
    return np.kron(up, up).T.astype(np.float32)


def dot(a, b):
    return jnp.dot(a, b, preferred_element_type=F32)


def dot_nt(a, b):
    return lax.dot_general(a, b, (((1,), (1,)), ((), ())), preferred_element_type=F32)


def pick(index, values):
    out = values[-1]
    for k in range(len(values) - 1):
        out = jnp.where(index == k, values[k], out)
    return out


def body(
    tok_h, quant_h, canvas_h, lift_h, loc_h, fac_h, sharp_s, qkv_h, wo_h, up_h, wd_h,
    kc_h, vc_h, fin_h, voc_h, kron_h,
    logits_o, canvas_o,
    tok, quant, canv, lift, loc, fac, kc, vc, fin, voc, kron,
    wq, wo, wu, wd,
    emb, st, nb1, nb2, nb3, qn, kn, vn, knc, att, attr, hid, pbuf, precv, pacc,
    load_sem, own_sem,
    qs, qr, us, ur, wos, wor, ats, atr, g2s, g2r, rss, rsr, g3s, g3r,
):
    me = lax.axis_index("tensor")
    dp = lax.axis_index("dp")
    mz = dp // 8
    my = lax.rem(dp // 2, 4)
    mc = lax.rem(dp, 2)
    right = lax.rem(me + 1, NX)
    left = lax.rem(me + 3, NX)
    opp = lax.rem(me + 2, NX)
    yp, ym, yo = lax.rem(my + 1, 4), lax.rem(my + 3, 4), lax.rem(my + 2, 4)
    zp, zm, zo = lax.rem(mz + 1, 4), lax.rem(mz + 3, 4), lax.rem(mz + 2, 4)

    def dpi(z, y, c):
        return {"dp": (z * 4 + y) * 2 + c}

    def rc(src, dst, s, r, dev):
        return pltpu.make_async_remote_copy(
            src_ref=src, dst_ref=dst, send_sem=s, recv_sem=r, device_id=dev, device_id_type=MESH
        )

    mycols = pl.ds(pl.multiple_of(me * LW, 128), LW)
    loads = [
        (tok_h, tok), (quant_h, quant), (canvas_h, canv), (lift_h, lift), (loc_h, loc),
        (fac_h, fac), (wo_h, wo.at[mz, my, mc, :, mycols]), (wd_h, wd.at[mz, my, mc]),
        (kc_h, kc), (vc_h, vc), (fin_h, fin), (voc_h, voc), (kron_h, kron),
    ]

    def load(k):
        return pltpu.make_async_copy(loads[k][0], loads[k][1], load_sem.at[k])

    own_q = [
        pltpu.make_async_copy(
            qkv_h.at[k], wq.at[mz, my, mc, :, pl.ds(k * LW, LW)], own_sem.at[1 + k]
        )
        for k in range(3)
    ]
    own_u = pltpu.make_async_copy(up_h, wu.at[mz, my, mc], own_sem.at[0])
    for c in own_q:
        c.start()
    for k in (6, 7, 0, 1, 12, 2, 3, 4, 5):
        load(k).start()
    own_u.start()
    for k in (8, 9, 10, 11):
        load(k).start()

    barrier = pltpu.get_barrier_semaphore()
    peers = [{"tensor": right}, {"tensor": left}, {"tensor": opp}]
    peers += [dpi(mz, yp, mc), dpi(mz, ym, mc), dpi(mz, yo, mc), dpi(zp, my, mc), dpi(zm, my, mc)]
    peers += [dpi(zo, my, mc), dpi(mz, my, 1 - mc)]
    for dev in peers:
        pl.semaphore_signal(barrier, inc=1, device_id=dev, device_id_type=MESH)
    pl.semaphore_wait(barrier, len(peers))

    weights = (wo, wu, wd)

    def ring(w, split, v, sends, recvs):
        c0, c1, ch = split[v]
        a, ap, am, ao = (my, yp, ym, yo) if v == 0 else (mz, zp, zm, zo)
        b, bp, bm, bo = (mz, zp, zm, zo) if v == 0 else (my, yp, ym, yo)

        def at(ai, bi, lo, hi, core=mc):
            cols = pl.ds(lo, hi - lo)
            return w.at[bi, ai, core, :, cols] if v == 0 else w.at[ai, bi, core, :, cols]

        def dev(ai, bi):
            return dpi(bi, ai, mc) if v == 0 else dpi(ai, bi, mc)

        def copy(k, src, to):
            return rc(src, src, sends.at[k], recvs.at[k], to)

        return c0, c1, ch, (a, ap, am, ao), (b, bp, bm, bo), at, dev, copy

    other = dpi(mz, my, 1 - mc)

    def qkv_copies(v):
        c0, c1, ch, (a, ap, am, ao), (b, bp, bm, bo), at, dev, copy = ring(
            wq, QKV_SPLIT, v, qs.at[v], qr.at[v]
        )
        every = slice(None)
        row = (a, am, ap, ao)
        send = [
            (at(a, b, c0, c1), dev(ap, b)),
            (at(a, b, c0, c1), dev(am, b)),
            (at(a, b, c0, ch), dev(ao, b)),
            (at(a, b, ch, c1), dev(ao, b)),
        ]
        recv = [at(am, b, c0, c1), at(ap, b, c0, c1), at(ao, b, c0, ch), at(ao, b, ch, c1)]
        send += [(at(ai, b, c0, c1), dev(a, bp)) for ai in row]
        recv += [at(ai, bm, c0, c1) for ai in row]
        send += [(at(ai, b, c0, c1), dev(a, bm)) for ai in row]
        recv += [at(ai, bp, c0, c1) for ai in row]
        send += [(at(ai, bm, c0, c1), dev(a, bp)) for ai in row[:2]]
        send += [(at(ai, bp, c0, c1), dev(a, bm)) for ai in row[2:]]
        recv += [at(ai, bo, c0, c1) for ai in row]
        send += [(at(every, bi, c0, c1), other) for bi in (b, bm, bp, bo)]
        recv += [at(every, bi, c0, c1, 1 - mc) for bi in (b, bm, bp, bo)]
        return (
            [lambda k=k, x=x: copy(k, *x) for k, x in enumerate(send)],
            [lambda k=k, x=x: copy(k, x, other) for k, x in enumerate(recv)],
        )

    QKV_STAGES = (
        (((), (0, 1, 2, 3, 4, 8)),),
        (((0,), (5, 9)), ((1,), (6, 10))),
        (((2, 3), (7, 11, 16)),),
        (((4,), (12,)), ((5,), (13,)), ((10,), (14,))),
        (((11,), (15,)), ((6, 7), (17,)), ((8, 9), (18,))),
        (((12, 13, 14, 15), (19,)),),
        (((16, 17, 18, 19), ()),),
    )

    def qkv_stage(k):
        for waits, starts in QKV_STAGES[k]:
            for v in (0, 1):
                send, recv = qkv_copies(v)
                for i in waits:
                    recv[i]().wait_recv()
                for i in starts:
                    send[i]().start()

    def unit_copies(r, v):
        w = weights[r]
        u = 2 * r + v
        c0, c1, ch, (a, ap, am, ao), (b, bp, bm, bo), at, dev, copy = ring(
            w, SPLIT, v, us.at[u], ur.at[u]
        )

        send = [
            lambda: copy(0, at(a, b, c0, c1), dev(ap, b)),
            lambda: copy(1, at(a, b, c0, c1), dev(am, b)),
            lambda: copy(2, at(am, b, c0, ch), dev(ap, b)),
            lambda: copy(3, at(ap, b, ch, c1), dev(am, b)),
            lambda: copy(4, at(slice(None), b, c0, c1), dev(a, bp)),
            lambda: copy(5, at(slice(None), b, c0, c1), dev(a, bm)),
            lambda: copy(6, at(pl.ds(0, 2), bm, c0, c1), dev(a, bp)),
            lambda: copy(7, at(pl.ds(2, 2), bp, c0, c1), dev(a, bm)),
            lambda: copy(8, w.at[:, :, mc, :, pl.ds(c0, c1 - c0)], other),
        ]
        recv = [
            lambda: copy(0, at(am, b, c0, c1), dev(ap, b)),
            lambda: copy(1, at(ap, b, c0, c1), dev(am, b)),
            lambda: copy(2, at(ao, b, c0, ch), dev(ap, b)),
            lambda: copy(3, at(ao, b, ch, c1), dev(am, b)),
            lambda: copy(4, at(slice(None), bm, c0, c1), dev(a, bp)),
            lambda: copy(5, at(slice(None), bp, c0, c1), dev(a, bm)),
            lambda: copy(6, at(pl.ds(0, 2), bo, c0, c1), dev(a, bp)),
            lambda: copy(7, at(pl.ds(2, 2), bo, c0, c1), dev(a, bm)),
            lambda: copy(8, w.at[:, :, 1 - mc, :, pl.ds(c0, c1 - c0)], other),
        ]
        return send, recv

    def step(r, k):
        for i in (0, 1):
            for v in (0, 1):
                send, recv = unit_copies(r, v)
                if k == 1:
                    send[i]().start()
                elif k in (2, 4):
                    recv[2 * k - 4 + i]().wait_recv()
                    send[2 * k - 2 + i]().start()
                elif k in (3, 5):
                    if i == 0:
                        recv[2 * k - 4]().wait_recv()
                        recv[2 * k - 3]().wait_recv()
                        if k == 5:
                            send[8]().start()
                    if k == 3:
                        send[4 + i]().start()
                elif k == 6 and i == 0:
                    recv[8]().wait_recv()

    for c in own_q:
        c.wait()
    qkv_stage(0)

    load(6).wait()
    load(7).wait()
    own_u.wait()
    step(1, 1)

    def wo_copy(k, owner, to):
        part = wo.at[mz, my, mc, :, pl.ds(pl.multiple_of(owner * LW, 128), LW)]
        return rc(part, part, wos.at[k], wor.at[k], {"tensor": to})

    wo_sends = [wo_copy(0, me, right), wo_copy(1, me, left), wo_copy(2, me, opp)]
    wo_recvs = [wo_copy(0, left, right), wo_copy(1, right, left), wo_copy(2, opp, opp)]
    for c in wo_sends:
        c.start()

    load(0).wait()
    load(1).wait()
    emb[...] = jnp.zeros_like(emb)

    def high_low(v):
        high = v.astype(BF)
        return high, (v - high.astype(F32)).astype(BF)

    def embed(n, carry):
        base = pl.multiple_of(n * 512, 512)
        table = jnp.concatenate(high_low(quant[:, pl.ds(base, 512)]), axis=0)
        ids = lax.broadcasted_iota(jnp.int32, (512, PREVTOK), 0) + base
        for j in range(IMGS):
            onehot = jnp.where(tok[j : j + 1, :] == ids, 1.0, 0.0).astype(BF)
            emb[j] += dot(table, onehot)
        return carry

    lax.fori_loop(0, 5, embed, 0)
    qkv_stage(1)
    step(2, 1)
    lax.fori_loop(5, 8, embed, 0)
    qkv_stage(2)
    for c in wo_recvs:
        c.wait_recv()
    step(0, 1)

    def modulated(rows_value, scale, shift):
        center = rows_value - jnp.mean(rows_value, axis=-1, keepdims=True)
        variance = jnp.mean(center * center, axis=-1, keepdims=True)
        return (center * lax.rsqrt(variance + FLOOR) * (1.0 + scale) + shift).astype(BF)

    for k in (12, 2, 3, 4, 5):
        load(k).wait()

    ORDER = (2, 1, 3, 0)

    def first_norm(jj, carry):
        j = lax.rem(me + pick(jj, ORDER), NX)
        rows = emb[j, 0:CVAE, :] + emb[j, CVAE : 2 * CVAE, :]
        lifted = lax.dot_general(
            rows, kron[...], (((1,), (0,)), ((), ())),
            precision=lax.Precision.HIGHEST, preferred_element_type=F32,
        )
        can = canv[j] + lifted
        canvas_o[j] = can
        can_hi, can_lo = high_low(can)
        can3 = jnp.concatenate([can_hi, can_lo, can_hi], axis=0)
        for n in range(3):
            cols = slice(n * 512, (n + 1) * 512)
            lift_hi, lift_lo = high_low(lift[:, cols])
            lift3 = jnp.concatenate([lift_hi, lift_hi, lift_lo], axis=0)
            st[:, cols] = loc[:, cols] + lax.dot_general(
                can3, lift3, (((0,), (0,)), ((), ())), preferred_element_type=F32
            )
        scale = fac[2, pl.ds(j, 1), :]
        shift = fac[4, pl.ds(j, 1), :]

        def rows_norm(m, c):
            r = pl.ds(pl.multiple_of(m * 64, 64), 64)
            nb1[j, r, :] = modulated(st[r, :], scale, shift)
            return c

        lax.fori_loop(0, 4, rows_norm, 0)

        @pl.when(jj == 0)
        def _():
            qkv_stage(3)
            step(0, 2)

        @pl.when(jj == 1)
        def _():
            qkv_stage(4)
            step(1, 2)
            step(0, 3)

        @pl.when(jj == 2)
        def _():
            step(2, 2)

        @pl.when(jj == 3)
        def _():
            qkv_stage(5)

        return carry

    lax.fori_loop(0, 4, first_norm, 0)

    load(8).wait()
    load(9).wait()

    def to_head(lanes):
        return (
            (lanes >= HDIM).astype(jnp.int32)
            + (lanes >= 2 * HDIM).astype(jnp.int32)
            + (lanes >= 3 * HDIM).astype(jnp.int32)
        )

    block_ones = jnp.where(to_head(lax.broadcasted_iota(jnp.int32, (LW, LW), 0))
        == to_head(lax.broadcasted_iota(jnp.int32, (LW, LW), 1)), 1.0, 0.0).astype(BF)
    lane_row = to_head(lax.broadcasted_iota(jnp.int32, (1, LW), 1))
    sharp = jnp.where(
        lane_row == 0,
        sharp_s[0, 0],
        jnp.where(lane_row == 1, sharp_s[0, 1], jnp.where(lane_row == 2, sharp_s[0, 2], sharp_s[0, 3])),
    )

    def unit(u):
        return u * lax.rsqrt(dot((u * u).astype(BF), block_ones) + 1.0)

    def cache_keys(j, carry):
        knc[j] = unit(kc[j].astype(F32)).astype(BF)
        return carry

    lax.fori_loop(0, 4, cache_keys, 0)
    qkv_stage(6)

    def att_copy(jj, owner, to):
        return rc(att.at[jj], attr.at[owner], ats.at[jj], atr.at[jj], {"tensor": to})

    def attend(jj, carry):
        off = pick(jj, ORDER)
        j = lax.rem(me + off, NX)
        x = nb1[j]
        q = dot(x, wq[:, :, :, :, 0:LW].reshape(D, LW))
        qn[...] = (unit(q) * sharp).astype(BF)
        k = dot(x, wq[:, :, :, :, LW : 2 * LW].reshape(D, LW))
        kn[...] = unit(k).astype(BF)
        vn[...] = dot(x, wq[:, :, :, :, 2 * LW : 3 * LW].reshape(D, LW)).astype(BF)
        @pl.when(jj == 0)
        def _():
            step(0, 4)
            step(1, 3)

        @pl.when(jj == 1)
        def _():
            step(2, 3)

        @pl.when(jj == 2)
        def _():
            step(0, 5)

        outs = []
        for h in range(HEADS_L):
            w0, w1 = WINDOWS[h]
            lanes = lax.broadcasted_iota(jnp.int32, (TOK, w1 - w0), 1) + w0
            mine = (lanes >= h * HDIM) & (lanes < (h + 1) * HDIM)
            qh = jnp.where(mine, qn[:, w0:w1], jnp.zeros((), BF))
            sc = dot_nt(qh, knc[j, :, w0:w1])
            sn = dot_nt(qh, kn[:, w0:w1])
            top = jnp.maximum(
                jnp.max(sc, axis=-1, keepdims=True), jnp.max(sn, axis=-1, keepdims=True)
            )
            pc = jnp.exp(sc - top)
            pn = jnp.exp(sn - top)
            total = jnp.sum(pc, axis=-1, keepdims=True) + jnp.sum(pn, axis=-1, keepdims=True)
            o = dot(pc.astype(BF), vc[j, :, w0:w1]) + dot(pn.astype(BF), vn[:, w0:w1])
            outs.append(o * (1.0 / total))
        lane = lax.broadcasted_iota(jnp.int32, (TOK, 128), 1)
        for c in range(3):
            w0 = WINDOWS[c + 1][0]
            first = outs[c][:, c * 128 - WINDOWS[c][0] : c * 128 - WINDOWS[c][0] + 128]
            second = outs[c + 1][:, c * 128 - w0 : c * 128 - w0 + 128]
            edge = (c + 1) * HDIM - c * 128
            att[jj, :, c * 128 : (c + 1) * 128] = jnp.where(lane < edge, first, second).astype(BF)

        @pl.when(jj < 3)
        def _():
            att_copy(jj, me, j).start()

        return carry

    lax.fori_loop(0, 4, attend, 0)
    attr[me] = att[3]
    for jj in range(3):
        att_copy(jj, lax.rem(me + 4 - ORDER[jj], NX), opp).wait_recv()
    step(0, 6)
    step(1, 4)

    def mix(z, carry):
        cols = pl.ds(pl.multiple_of(z * LW, 128), LW)
        mixed = jnp.zeros((TOK, LW), F32)
        for g in range(NX):
            w = wo[z, :, :, :, g * LW : (g + 1) * LW].reshape(LW, LW)
            mixed = mixed + dot_nt(attr[g], w).astype(BF).astype(F32)
        st[:, cols] = st[:, cols] + fac[0, pl.ds(me, 1), cols] * mixed
        return carry

    lax.fori_loop(0, 4, mix, 0)

    scale2 = fac[3, pl.ds(me, 1), :]
    shift2 = fac[5, pl.ds(me, 1), :]

    def second_norm(m, c):
        r = pl.ds(pl.multiple_of(m * 64, 64), 64)
        nb2[me, r, :] = modulated(st[r, :], scale2, shift2)
        return c

    def rows_at(first, count):
        return pl.ds(first, count)

    def gather_copies(nb, ss, rs):
        def c(k, img, first, count, to):
            ref = nb.at[img, rows_at(first, count), :]
            return rc(ref, ref, ss.at[k], rs.at[k], {"tensor": to})

        send, recv = [], []
        for k, first in ((0, 0), (2, HALF)):
            send += [c(k, me, first, HALF, right), c(k + 1, me, first, HALF, left)]
            recv += [c(k, left, first, HALF, right), c(k + 1, right, first, HALF, left)]
        for k, first in ((4, 0), (6, HALF)):
            send += [c(k, left, first, QUART, right), c(k + 1, right, first + QUART, QUART, left)]
            recv += [c(k, opp, first, QUART, right), c(k + 1, opp, first + QUART, QUART, left)]
        return send, recv

    def pass_on(b, send, recv):
        for i in (0, 1):
            recv[2 * b + i].wait_recv()
            send[4 + 2 * b + i].start()

    def blocks(s):
        ia = lax.rem(me + pick(s, (0, 3, 3, 2)), NX)
        ib = lax.rem(me + pick(s, (0, 1, 1, 2)), NX)
        ha = pick(s, (0, 0, 1, 0))
        hb = pick(s, (1, 0, 1, 1))
        ra = pl.ds(pl.multiple_of(ha * HALF, HALF), HALF)
        rb = pl.ds(pl.multiple_of(hb * HALF, HALF), HALF)
        return ia, ra, ib, rb

    send2, recv2 = gather_copies(nb2, g2s, g2r)
    for b in (0, 1):
        lax.fori_loop(2 * b, 2 * b + 2, second_norm, 0)
        send2[2 * b].start()
        send2[2 * b + 1].start()
    step(2, 4)
    step(1, 5)

    def part(k, src, dst, to):
        return rc(src, dst, rss.at[k], rsr.at[k], {"tensor": to})

    def partial_copies(b):
        f = b * HALF
        mine = pbuf.at[1 + b]
        far = pbuf.at[3]
        low, high = rows_at(f, QUART), rows_at(f + QUART, QUART)
        k = 6 * b
        send = [
            part(k, mine.at[rows_at(HALF + QUART, QUART), :], precv.at[0, high, :], right),
            part(k + 1, mine.at[rows_at(0, QUART), :], precv.at[1, low, :], left),
            part(k + 2, far.at[low, :], pacc.at[0, rows_at(b * QUART, QUART), :], right),
            part(k + 3, far.at[high, :], pacc.at[1, rows_at(b * QUART, QUART), :], left),
            part(k + 4, mine.at[rows_at(HALF, QUART), :], precv.at[0, low, :], right),
            part(k + 5, mine.at[rows_at(QUART, QUART), :], precv.at[1, high, :], left),
        ]
        return send

    parts = [partial_copies(b) for b in (0, 1)]

    def widen(s):
        ia, ra, ib, rb = blocks(s)

        def tile(n, c):
            cols = pl.ds(pl.multiple_of(n * LW, 128), LW)
            x = jnp.concatenate([nb2[ia, ra, :], nb2[ib, rb, :]], axis=0)
            u = dot(x, wu[:, :, :, :, cols].reshape(D, LW))
            act = 0.5 * u * (1.0 + jnp.tanh(0.7978845608028654 * (u + 0.044715 * (u * u * u))))
            hid[s, :, cols] = act.astype(BF)
            return c

        lax.fori_loop(0, 4, tile, 0)

    def narrow(s):
        def tile(z, c):
            cols = pl.ds(pl.multiple_of(z * LW, 128), LW)
            pbuf[s, :, cols] = dot_nt(hid[s], wd[z].reshape(LW, D)).astype(BF)
            return c

        lax.fori_loop(0, 4, tile, 0)

    pass_on(0, send2, recv2)
    step(1, 6)

    def widen_ready(t, carry):
        s = pick(t, (1, 0, 2, 3))

        @pl.when(t == 1)
        def _():
            step(2, 5)

        @pl.when(t == 2)
        def _():
            pass_on(1, send2, recv2)

        @pl.when(t == 3)
        def _():
            step(2, 6)

            def near(s, c):
                narrow(s)
                return c

            lax.fori_loop(1, 3, near, 0)
            for b in (0, 1):
                parts[b][0].start()
                parts[b][1].start()
            for k in range(4, 8):
                recv2[k].wait_recv()

        widen(s)
        return carry

    lax.fori_loop(0, 4, widen_ready, 0)

    def narrow_last(t, carry):
        @pl.when(t == 1)
        def _():
            for b in (0, 1):
                parts[b][2].start()
                parts[b][3].start()

        narrow(pick(t, (3, 0)))
        return carry

    lax.fori_loop(0, 2, narrow_last, 0)
    load(10).wait()
    load(11).wait()

    for b in (0, 1):
        came = rows_at(b * QUART, QUART)
        for side, first in ((0, HALF), (1, QUART)):
            parts[b][2 + side].wait_recv()
            rows = rows_at(first, QUART)
            pbuf[1 + b, rows, :] = (
                pbuf[1 + b, rows, :].astype(F32) + pacc[side, came, :].astype(F32)
            ).astype(BF)
            parts[b][4 + side].start()

    gamma2 = fac[1, pl.ds(me, 1), :]
    scale3 = fin[me, 0:1, :]
    shift3 = fin[me, 1:2, :]

    def third_norm(m, c):
        r = pl.ds(pl.multiple_of(m * 64, 64), 64)
        mixed = pbuf[0, r, :].astype(F32) + precv[0, r, :].astype(F32) + precv[1, r, :].astype(F32)
        nb3[me, r, :] = modulated(st[r, :] + gamma2 * mixed, scale3, shift3)
        return c

    send3, recv3 = gather_copies(nb3, g3s, g3r)
    for b in (0, 1):
        for k in (0, 1, 4, 5):
            parts[b][k].wait_recv()
        lax.fori_loop(2 * b, 2 * b + 2, third_norm, 0)
        send3[2 * b].start()
        send3[2 * b + 1].start()

    def head(s, carry):
        @pl.when(s == 1)
        def _():
            pass_on(0, send3, recv3)

        @pl.when(s == 2)
        def _():
            pass_on(1, send3, recv3)

        ia, ra, ib, rb = blocks(s)

        def tile(n, c):
            cols = pl.ds(pl.multiple_of(n * 256, 256), 256)
            x = jnp.concatenate([nb3[ia, ra, :], nb3[ib, rb, :]], axis=0)
            y = dot(x, voc[:, cols]).astype(BF)
            logits_o[ia, ra, cols] = y[:HALF]
            logits_o[ib, rb, cols] = y[HALF:]
            return c

        lax.fori_loop(0, 4, tile, 0)
        return carry

    lax.fori_loop(0, 3, head, 0)
    for b in (0, 1):
        recv3[4 + 2 * b].wait_recv()
        recv3[5 + 2 * b].wait_recv()
        rows = rows_at(b * HALF, HALF)

        def last_tile(n, c):
            cols = pl.ds(pl.multiple_of(n * 256, 256), 256)
            logits_o[opp, rows, cols] = dot(nb3[opp, rows, :], voc[:, cols]).astype(BF)
            return c

        lax.fori_loop(0, 4, last_tile, 0)

    for v in (0, 1):
        send, _ = qkv_copies(v)
        for c in send:
            c().wait_send()
    for r in range(3):
        for v in (0, 1):
            send, _ = unit_copies(r, v)
            for k in range(9):
                send[k]().wait_send()
    for c in wo_sends:
        c.wait_send()
    for jj in range(3):
        att_copy(jj, me, opp).wait_send()
    for k in range(8):
        send2[k].wait_send()
        send3[k].wait_send()
    for b in (0, 1):
        for c in parts[b]:
            c.wait_send()


def local(
    sampled_earlier_tokens,
    quantizer_vectors,
    summed_latent_canvas,
    latent_lift_matrix,
    location_tier_offset,
    adaptive_norm_factors,
    logit_sharpness,
    probe_match_content_matrix,
    mixing_projection_matrix,
    widening_projection_matrix,
    narrowing_projection_matrix,
    cached_lower_grid_lookups,
    cached_lower_grid_payloads,
    final_norm_factors,
    vocabulary_logit_matrix,
):
    operands = (
        sampled_earlier_tokens,
        quantizer_vectors.T,
        jnp.swapaxes(summed_latent_canvas, 1, 2),
        latent_lift_matrix,
        location_tier_offset,
        jnp.swapaxes(adaptive_norm_factors[0], 0, 1),
        logit_sharpness,
        jnp.swapaxes(probe_match_content_matrix[0], 0, 1),
        mixing_projection_matrix[0].T,
        widening_projection_matrix[0],
        narrowing_projection_matrix[0].T,
        cached_lower_grid_lookups[0],
        cached_lower_grid_payloads[0],
        final_norm_factors,
        vocabulary_logit_matrix,
        jnp.asarray(upsample_matrix()),
    )
    anyspace = pl.BlockSpec(memory_space=pl.ANY)
    specs = [anyspace] * len(operands)
    specs[6] = pl.BlockSpec(memory_space=pltpu.SMEM)
    vm = pltpu.VMEM
    dma = pltpu.SemaphoreType.DMA
    scratch = [
        vm((IMGS, PREVTOK), jnp.int32),
        vm((CVAE, VOCAB), F32),
        vm((IMGS, CVAE, TOK), F32),
        vm((CVAE, D), F32),
        vm((TOK, D), F32),
        vm((6, IMGS, D), F32),
        vm((IMGS, CACHE, LW), BF),
        vm((IMGS, CACHE, LW), BF),
        vm((IMGS, 2, D), F32),
        vm((D, VL), BF),
        vm((PREVTOK, TOK), F32),
        vm((4, 4, 2, SH, 3 * LW), BF),
        vm((4, 4, 2, SH, D), BF),
        vm((4, 4, 2, SH, D), BF),
        vm((4, 4, 2, SH, D), BF),
        vm((IMGS, 2 * CVAE, PREVTOK), F32),
        vm((TOK, D), F32),
        vm((IMGS, TOK, D), BF),
        vm((IMGS, TOK, D), BF),
        vm((IMGS, TOK, D), BF),
        vm((TOK, LW), BF),
        vm((TOK, LW), BF),
        vm((TOK, LW), BF),
        vm((IMGS, CACHE, LW), BF),
        vm((NX, TOK, LW), BF),
        vm((NX, TOK, LW), BF),
        vm((NX, TOK, D), BF),
        vm((NX, TOK, D), BF),
        vm((2, TOK, D), BF),
        vm((2, HALF, D), BF),
        dma((13,)), dma((4,)),
        dma((2, 20)), dma((2, 20)), dma((6, 9)), dma((6, 9)), dma((3,)), dma((3,)), dma((3,)), dma((3,)),
        dma((8,)), dma((8,)), dma((12,)), dma((12,)), dma((8,)), dma((8,)),
    ]
    logits, canvas = pl.pallas_call(
        body,
        out_shape=(
            pltpu.VMEM((IMGS, TOK, VL), BF),
            pltpu.VMEM((IMGS, CVAE, TOK), F32),
        ),
        in_specs=specs,
        out_specs=(pl.BlockSpec(memory_space=pltpu.VMEM), pl.BlockSpec(memory_space=pltpu.VMEM)),
        scratch_shapes=scratch,
        compiler_params=pltpu.CompilerParams(
            collective_id=0, has_side_effects=True, vmem_limit_bytes=60_000_000
        ),
    )(*operands)
    return logits, jnp.swapaxes(canvas, 1, 2)


def solution(mesh):
    placed = (
        P("dp", None),
        P(),
        P("dp", None, None),
        P(),
        P(),
        P(None, "dp", None, None),
        P(None, "tensor"),
        P(None, "dp", None, "tensor"),
        P(None, "tensor", "dp"),
        P(None, "dp", "tensor"),
        P(None, "tensor", "dp"),
        P(None, "dp", None, "tensor"),
        P(None, "dp", None, "tensor"),
        P("dp", None, None),
        P(None, "tensor"),
    )
    return jax.shard_map(
        local,
        mesh=mesh,
        in_specs=placed,
        out_specs=(P("dp", None, "tensor"), P("dp", None, None)),
        check_vma=False,
    )
```
